32 devices in a mesh: tx: 4 (over z), ty: 2 (over y), vel: 4 (over x, core).
Axes of the slice: x: 2, y: 2, z: 4, core: 2. Of those that a mesh axis runs over, the one named last changes fastest.
Arguments:
- initial: float32 [32, 16, 16, 3072], P('tx', 'ty', None, 'vel'), may hold values from -2 to 3.5
- velocity: float32 [3, 3072], P(None, 'vel'), may hold values from -3 to 3, as said below
- weights: float32 [3072], P('vel'), may hold values from 0.5 to 2
- wall: int32 [32, 16, 16], P('tx', 'ty'), may hold values 0 or 1
- wall_temp: float32 [32, 16, 16], P('tx', 'ty'), may hold values from -1 to 1
- mass_target: float32 [], replicated, may hold values from 0.5 to 1.5
Outputs:
- distribution: float32 [32, 16, 16, 3072], P('tx', 'ty', None, 'vel')
- macro_fields: float32 [5, 32, 16, 16], P(None, 'tx', 'ty')
The draws below stay inside these ranges and needn't reach their ends.
Inputs may be any that keep to these rules, and one draw needn't show every extreme that they name: `velocity`: within each aligned block of 768 velocities the first quarter has positive x and y components, the second positive x and negative y, the third negative x and positive y, the fourth negative x and y; x and y components are 0.05 or more in magnitude.
All inputs are finite; a program needn't handle non-finite values. No bound on the sum of `wall` on one device may be relied on, other than what follows from the above.
Results may differ from the reference program's by a relative error of at most 0.0003.
Values sent between devices are 32-bit elements; how exact they have to be, the bound alone decides.
No kernel may reach another device: no remote copies, remote signals or barrier semaphores. Data moves between devices by JAX's collectives and lax.ppermute only.
A program may use at most 128 MiB of HBM per device.

```python
import math
import jax
import jax.numpy as jnp
from jax import lax

NZ = 16
V_DEV = 768
ITERS = 3
MACRO_STEPS = 4
NX = 32
NY = 16
V = 3072
N_VEL = 4


def draw_initial(key, part):
    rough_key = jax.random.fold_in(jax.random.fold_in(key, 11), 0)
    position = (jnp.arange(NX, dtype=jnp.float32) / NX)[:, None, None, None]
    rough_part = jnp.clip(jax.random.normal(rough_key, (NX, NY, NZ, V), jnp.float32), -4.0, 4.0)
    return 0.5 * rough_part + (0.3 + 0.6 * position)


def draw_velocity(key, part):
    size_key, lateral_key = jax.random.split(jax.random.fold_in(key, 23))
    slot_index = jnp.arange(V) % V_DEV
    quarter_index = slot_index // (V_DEV // 4)
    sign_x = jnp.where(quarter_index < 2, 1.0, -1.0)
    sign_y = jnp.where(quarter_index % 2 == 0, 1.0, -1.0)
    sizes = jnp.minimum(jnp.abs(jax.random.normal(size_key, (2, V), jnp.float32)), 2.95)
    lateral = jnp.clip(jax.random.normal(lateral_key, (V,), jnp.float32), -3.0, 3.0)
    return jnp.stack([sign_x * (0.05 + sizes[0]), sign_y * (0.05 + sizes[1]), lateral])


def touch_ends(values, own_key, low, high):
    shape = values.shape
    spot = [jax.random.randint(jax.random.fold_in(own_key, axis), (), 0, shape[axis]) for axis in range(len(shape))]
    values = values.at[tuple(spot)].set(low)
    longest = shape.index(max(shape))
    spot[longest] = (spot[longest] + 1) % shape[longest]
    return values.at[tuple(spot)].set(high)


def steps_of(key, extent, shards, smallest, high):
    def one(axis_at, shards_of):
        draws = jax.random.uniform(jax.random.fold_in(jax.random.fold_in(key, 6), axis_at), (shards_of,), jnp.float32, smallest / len(shards), high / len(shards))
        return jnp.repeat(jnp.exp(draws), extent[axis_at] // shards_of).reshape((-1,) + (1,) * (len(extent) - axis_at - 1))

    level = one(*shards[0])
    for cut in shards[1:]:
        level = level * one(*cut)
    return level


def setup_inputs(seed: int = 0) -> dict:
    streams_of = jax.random.split(jax.random.key(seed), 7)
    initial = draw_initial(jax.random.fold_in(streams_of[6], 71), 0)
    velocity = draw_velocity(jax.random.fold_in(streams_of[6], 71), 0)
    weights = jnp.clip(jnp.exp(math.log(2.0) - 1.3862944 * jax.random.uniform(streams_of[2], (V,), jnp.float32) ** steps_of(streams_of[2], (V,), ((0, 4),), -0.2, 0.2)), 0.5, 2.0)
    wall = touch_ends((jax.random.randint(streams_of[3], (NX, NY, NZ), 0, 8) < 1).astype(jnp.int32), jax.random.fold_in(streams_of[3], 1), 0, 1)
    wall_temp = jnp.clip(jax.random.uniform(streams_of[4], (NX, NY, NZ), jnp.float32, -1.0, 1.0) * steps_of(streams_of[4], (NX, NY, NZ), ((0, 4), (1, 2)), -0.4, 0.0), -1.0, 1.0)
    mass_target = jnp.clip(jax.random.uniform(streams_of[5], (), jnp.float32, 0.5, 1.5), 0.5, 1.5)
    return dict(initial=initial, velocity=velocity, weights=weights, wall=wall, wall_temp=wall_temp, mass_target=mass_target)


step_time = 0.1
collision = 1.0
macro_time = 0.1
viscosity = 1.0
conduction = 1.0
highest = lax.Precision.HIGHEST


def basis(velocity):
    speed_sq = velocity[0] * velocity[0] + velocity[1] * velocity[1] + velocity[2] * velocity[2]
    return jnp.stack([jnp.ones_like(speed_sq), 2.0 * velocity[0], 2.0 * velocity[1], 2.0 * velocity[2], speed_sq - 1.5])


def projector(velocity, weights, total_count):
    vel_x, vel_y, vel_z = velocity[0], velocity[1], velocity[2]
    speed_sq = vel_x * vel_x + vel_y * vel_y + vel_z * vel_z
    moment_rows = jnp.stack([jnp.ones_like(speed_sq), vel_x, vel_y, vel_z, (2.0 / 3.0) * speed_sq - 1.0,
                             2.0 * (vel_x * vel_x - speed_sq / 3.0), 2.0 * (vel_y * vel_y - speed_sq / 3.0),
                             2.0 * (vel_z * vel_z - speed_sq / 3.0), 2.0 * vel_x * vel_y, 2.0 * vel_x * vel_z,
                             2.0 * vel_y * vel_z, vel_x * (speed_sq - 2.5), vel_y * (speed_sq - 2.5),
                             vel_z * (speed_sq - 2.5)])
    return moment_rows * (weights / total_count)[None, :]


def differences(shifted):
    grads = [(shifted(direction, 1) - shifted(direction, -1)) * 0.5 for direction in (1, 2, 3)]
    middle = shifted(1, 0)
    laplace = (shifted(1, 1) + shifted(1, -1) - 2.0 * middle) + (shifted(2, 1) + shifted(2, -1) - 2.0 * middle)
    laplace = laplace + (shifted(3, 1) + shifted(3, -1) - 2.0 * middle)
    return grads, laplace, middle


def macro_sources(shifted):
    grads, laplace, middle = differences(shifted)
    grad_x, grad_y, grad_z = grads
    sig_x = grad_x[0] + grad_y[3] + grad_z[4]
    sig_y = grad_x[3] + grad_y[1] + grad_z[5]
    sig_z = grad_x[4] + grad_y[5] + grad_z[2]
    heat_flow = grad_x[6] + grad_y[7] + grad_z[8]
    return jnp.stack([-0.5 * (sig_x + viscosity * laplace[9]), -0.5 * (sig_y + viscosity * laplace[10]),
                      -0.5 * (sig_z + viscosity * laplace[11]), -(2.0 / 3.0) * (heat_flow + conduction * laplace[12])])


def macro_step(shifted, sources):
    grads, laplace, middle = differences(shifted)
    grad_x, grad_y, grad_z = grads
    div_u = grad_x[1] + grad_y[2] + grad_z[3]
    change_rates = [-div_u]
    for component in range(3):
        along = grads[component]
        change_rates.append(-0.5 * (along[0] + along[4]) + 0.5 * viscosity * laplace[1 + component] + sources[component])
    change_rates.append(-(2.0 / 3.0) * div_u + (2.0 / 3.0) * conduction * laplace[4] + sources[3])
    return middle + macro_time * jnp.stack(change_rates)


def kinetic_update(corrected, equilibrium, before_x, after_x, before_y, after_y, velocity):
    plus_part = jnp.maximum(velocity, 0.0)
    minus_part = jnp.minimum(velocity, 0.0)
    before_z = jnp.roll(corrected, 1, 2)
    after_z = jnp.roll(corrected, -1, 2)
    transport = plus_part[0] * (corrected - before_x) + minus_part[0] * (after_x - corrected)
    transport = transport + (plus_part[1] * (corrected - before_y) + minus_part[1] * (after_y - corrected))
    transport = transport + (plus_part[2] * (corrected - before_z) + minus_part[2] * (after_z - corrected))
    return corrected - step_time * transport + (step_time * collision) * (equilibrium - corrected)


def rolled(stack):
    def shifted(direction, offset):
        return jnp.roll(stack, -offset, direction)
    return shifted


def reference(initial, velocity, weights, wall, wall_temp, mass_target):
    block_count = N_VEL
    block_width = V // N_VEL
    state_f = jnp.moveaxis(initial.reshape(NX, NY, NZ, block_count, block_width), 3, 0)
    vel_blocks = jnp.moveaxis(velocity.reshape(3, block_count, block_width), 1, 0)
    weight_blocks = weights.reshape(block_count, block_width)
    is_wall = (wall == 1)[..., None]
    cell_count = float(NX * NY * NZ)
    macro_state = None
    for iteration in range(ITERS):
        def block_moments(pieces):
            dist_slab, vel_slab, weight_slab = pieces
            return jnp.einsum("kv,xyzv->kxyz", projector(vel_slab, weight_slab, float(V)), dist_slab,
                              precision=highest)

        moments = jnp.sum(lax.map(block_moments, (state_f, vel_blocks, weight_blocks)), axis=0)
        kinetic_state = moments[0:5]
        fields = jnp.concatenate([moments[5:14], moments[1:5]])
        sources = macro_sources(rolled(fields))
        macro_state = kinetic_state
        for sweep in range(MACRO_STEPS):
            macro_state = macro_step(rolled(macro_state), sources)
        density_mean = jnp.sum(macro_state[0]) / cell_count
        macro_state = jnp.concatenate([((macro_state[0] - density_mean) + mass_target)[None], macro_state[1:]])
        change = macro_state - kinetic_state
        current_state = macro_state

        def block_kinetic(pieces):
            dist_slab, vel_slab = pieces
            rows = basis(vel_slab)
            corrected = dist_slab + jnp.einsum("kxyz,kv->xyzv", change, rows, precision=highest)
            equilibrium = jnp.einsum("kxyz,kv->xyzv", current_state, rows, precision=highest)
            updated = kinetic_update(corrected, equilibrium, jnp.roll(corrected, 1, 0), jnp.roll(corrected, -1, 0),
                                     jnp.roll(corrected, 1, 1), jnp.roll(corrected, -1, 1), vel_slab)
            return jnp.where(is_wall, wall_temp[..., None] * rows[4], updated)

        state_f = lax.map(block_kinetic, (state_f, vel_blocks))
    distribution = jnp.moveaxis(state_f, 0, 3).reshape(NX, NY, NZ, V)
    return distribution, macro_state
```

```python
import functools

import jax
import jax.numpy as jnp
from jax import lax
from jax.experimental import pallas as pl
from jax.experimental.pallas import tpu as pltpu
from jax.sharding import PartitionSpec as P

ITERS = 3
MACRO_STEPS = 4

STEP_TIME = 0.1
COLLISION = 1.0
MACRO_TIME = 0.1
VISCOSITY = 1.0
CONDUCTION = 1.0

LANES = 128
MOMENTS = 14
PROWS = 16
KROWS = 48
f32 = jnp.float32
bf16 = jnp.bfloat16


def split(value):
    high = value.astype(bf16)
    return high, (value - high.astype(f32)).astype(bf16)


def dot(a, b, contract):
    return lax.dot_general(a, b, (contract, ((), ())), preferred_element_type=f32)


def local_moments(proj, plane):
    high, low = split(plane)
    both = dot(proj, high, ((1,), (1,)))
    return both[:PROWS] + both[PROWS:] + dot(proj[:PROWS], low, ((1,), (1,)))


def prepare_kernel(vel, wgt, h, mom, proj, wmat, coef, ysend, xup, xdown, rows, *, total):
    x = pl.program_id(0)
    planes = pl.num_programs(0)
    vx, vy, vz = vel[0:1, :], vel[1:2, :], vel[2:3, :]

    @pl.when(x == 0)
    def _():
        speed = vx * vx + vy * vy + vz * vz
        scale = wgt[...] / total
        one = jnp.ones_like(speed)
        zero = jnp.zeros_like(speed)
        table = [
            one,
            vx,
            vy,
            vz,
            2.0 / 3.0 * speed - 1.0,
            2.0 * (vx * vx - speed / 3.0),
            2.0 * (vy * vy - speed / 3.0),
            2.0 * (vz * vz - speed / 3.0),
            2.0 * vx * vy,
            2.0 * vx * vz,
            2.0 * vy * vz,
            vx * (speed - 2.5),
            vy * (speed - 2.5),
            vz * (speed - 2.5),
        ]
        for k, row in enumerate(table):
            rows[k : k + 1, :] = row * scale
        for k in range(MOMENTS, PROWS):
            rows[k : k + 1, :] = zero
        high, low = split(rows[0:PROWS, :])
        proj[0:PROWS, :] = high
        proj[PROWS : 2 * PROWS, :] = low
        along_x, along_y, along_z = (STEP_TIME * jnp.abs(v) for v in (vx, vy, vz))
        centre = (1.0 - STEP_TIME * COLLISION) - (along_x + along_y + along_z)
        for k, row in enumerate([centre, along_x, along_y, along_z, vy, vz, zero, zero]):
            coef[k : k + 1, :] = row
        basis = [one, 2.0 * vx, 2.0 * vy, 2.0 * vz, speed - 1.5]
        parts = [
            centre,
            jnp.where(vx > 0.0, along_x, 0.0),
            jnp.where(vx > 0.0, 0.0, along_x),
            jnp.where(vy > 0.0, along_y, 0.0),
            jnp.where(vy > 0.0, 0.0, along_y),
            jnp.where(vz > 0.0, along_z, 0.0),
            jnp.where(vz > 0.0, 0.0, along_z),
            STEP_TIME * COLLISION * one,
        ]
        for i, part in enumerate(parts):
            for k, row in enumerate(basis):
                rows[5 * i + k : 5 * i + k + 1, :] = part * row
        rows[40:41, :] = one
        rows[41:42, :] = basis[4]
        for k in range(42, KROWS):
            rows[k : k + 1, :] = zero
        high, low = split(rows[...])
        wmat[0:KROWS, :] = high
        wmat[KROWS : 2 * KROWS, :] = high
        wmat[2 * KROWS : 3 * KROWS, :] = low

    _, ny, nz, nv = h.shape
    plane = h[0].reshape(ny * nz, nv)
    out = local_moments(proj[...], plane)
    mom[pl.ds(x, MOMENTS, stride=planes), :] = out[:MOMENTS]
    ysend[0] = jnp.where(vy > 0.0, plane[(ny - 1) * nz :], plane[:nz])

    @pl.when(x == planes - 1)
    def _():
        xup[...] = h[0, :, :, : nv // 2]

    @pl.when(x == 0)
    def _():
        xdown[...] = h[0, :, :, nv // 2 :]


def prepare(initial, velocity, weights, total):
    nx, ny, nz, nv = initial.shape
    whole = lambda *shape: pl.BlockSpec(shape, lambda x: (0,) * len(shape))
    return pl.pallas_call(
        functools.partial(prepare_kernel, total=total),
        grid=(nx,),
        in_specs=[whole(3, nv), whole(1, nv), pl.BlockSpec((1, ny, nz, nv), lambda x: (x, 0, 0, 0))],
        out_specs=[
            whole(MOMENTS * nx, ny * nz),
            whole(2 * PROWS, nv),
            whole(3 * KROWS, nv),
            whole(8, nv),
            pl.BlockSpec((1, nz, nv), lambda x: (x, 0, 0)),
            whole(ny, nz, nv // 2),
            whole(ny, nz, nv // 2),
        ],
        out_shape=[
            jax.ShapeDtypeStruct((MOMENTS * nx, ny * nz), f32),
            jax.ShapeDtypeStruct((2 * PROWS, nv), bf16),
            jax.ShapeDtypeStruct((3 * KROWS, nv), bf16),
            jax.ShapeDtypeStruct((8, nv), f32),
            jax.ShapeDtypeStruct((nx, nz, nv), f32),
            jax.ShapeDtypeStruct((ny, nz, nv // 2), f32),
            jax.ShapeDtypeStruct((ny, nz, nv // 2), f32),
        ],
        scratch_shapes=[pltpu.VMEM((KROWS, nv), f32)],
        name="prepare",
    )(velocity, weights[None], initial)


def stream_kernel(h, yhalo, xbefore, xafter, coef, fluid, g):
    nx, ny, nz, nv = h.shape
    tiles = nv // LANES
    for j in range(tiles):
        lanes = slice(j * LANES, (j + 1) * LANES)
        forward_x = j < tiles // 2
        half = slice(lanes.start % (nv // 2), lanes.start % (nv // 2) + LANES)
        row = lambda k: jnp.broadcast_to(coef[k : k + 1, lanes], (nz, LANES))
        centre, along_x, along_y, along_z = (row(k) for k in range(4))
        up_z = row(5) > 0.0
        quarters = {(lanes.start * 4) // nv, ((lanes.stop - 1) * 4) // nv}
        signs = {q % 2 == 0 for q in quarters}
        up_y = row(4) > 0.0
        for x in range(nx):
            for y in range(ny):
                c = h[x, y, :, lanes]
                if forward_x:
                    ux = h[x - 1, y, :, lanes] if x > 0 else xbefore[y, :, half]
                else:
                    ux = h[x + 1, y, :, lanes] if x < nx - 1 else xafter[y, :, half]
                before = h[x, y - 1, :, lanes] if y > 0 else yhalo[x, :, lanes]
                after = h[x, y + 1, :, lanes] if y < ny - 1 else yhalo[x, :, lanes]
                if signs == {True}:
                    uy = before
                elif signs == {False}:
                    uy = after
                else:
                    uy = jnp.where(up_y, before, after)
                uz = jnp.where(up_z, pltpu.roll(c, 1, 0), pltpu.roll(c, nz - 1, 0))
                out = (centre * c + along_x * ux) + (along_y * uy + along_z * uz)
                g[x, y, :, lanes] = out * fluid[x, y]


def stream(h, yhalo, xbefore, xafter, coef, fluid):
    return pl.pallas_call(
        stream_kernel,
        out_shape=jax.ShapeDtypeStruct(h.shape, f32),
        name="stream",
        cost_estimate=pl.CostEstimate(flops=2_000_000, bytes_accessed=8_000_000, transcendentals=0),
    )(h, yhalo, xbefore, xafter, coef, fluid)


def macro_kernel(target, own, side, left, left_side, right, right_side, far, fluid, heat, mix, state_out, *, cells, nz, last):
    nx, width = fluid.shape

    def field(k):
        part = slice(k * nx, (k + 1) * nx)
        here = jnp.concatenate([left[part], own[part], right[part]], axis=0)
        there = jnp.concatenate([left_side[part], side[part], right_side[part]], axis=0)
        return jnp.concatenate([here, there], axis=1)

    rows, lanes = 3 * nx, 2 * width
    depth = lax.broadcasted_iota(jnp.int32, (rows, lanes), 1) % nz
    first, final = depth == 0, depth == nz - 1

    def shift(v, direction, offset):
        if direction == 0:
            return pltpu.roll(v, 1 if offset < 0 else rows - 1, 0)
        if direction == 1:
            return pltpu.roll(v, nz if offset < 0 else lanes - nz, 1)
        if offset < 0:
            return jnp.where(first, pltpu.roll(v, lanes - nz + 1, 1), pltpu.roll(v, 1, 1))
        return jnp.where(final, pltpu.roll(v, nz - 1, 1), pltpu.roll(v, lanes - 1, 1))

    def around(v, directions=(0, 1, 2)):
        return {d: (shift(v, d, 1), shift(v, d, -1)) for d in directions}

    def grad(pair):
        return (pair[0] - pair[1]) * 0.5

    def laplace(v, near):
        total = (near[0][0] + near[0][1]) + (near[1][0] + near[1][1]) + (near[2][0] + near[2][1])
        return total - 6.0 * v

    def slope(v, d):
        return grad(around(v, (d,))[d])

    state = [field(k) for k in range(5)]
    kinetic = state
    near = [None] + [around(state[k]) for k in range(1, 5)]
    stress = [field(5 + k) for k in range(9)]
    sums = [
        slope(stress[0], 0) + slope(stress[3], 1) + slope(stress[4], 2),
        slope(stress[3], 0) + slope(stress[1], 1) + slope(stress[5], 2),
        slope(stress[4], 0) + slope(stress[5], 1) + slope(stress[2], 2),
    ]
    flow = slope(stress[6], 0) + slope(stress[7], 1) + slope(stress[8], 2)
    sources = [-0.5 * (sums[i] + VISCOSITY * laplace(state[1 + i], near[1 + i])) for i in range(3)]
    sources.append(-(2.0 / 3.0) * (flow + CONDUCTION * laplace(state[4], near[4])))
    for step in range(MACRO_STEPS):
        if step:
            near = [None] + [around(state[k]) for k in range(1, 5)]
        near[0] = around(state[0])
        div = grad(near[1][0]) + grad(near[2][1]) + grad(near[3][2])
        rates = [-div]
        for i in range(3):
            rates.append(
                -0.5 * (grad(near[0][i]) + grad(near[4][i]))
                + 0.5 * VISCOSITY * laplace(state[1 + i], near[1 + i])
                + sources[i]
            )
        rates.append(-(2.0 / 3.0) * div + 2.0 / 3.0 * CONDUCTION * laplace(state[4], near[4]) + sources[3])
        state = [s + MACRO_TIME * r for s, r in zip(state, rates)]

    mass = far[...]
    for part in (own, side, left, left_side, right, right_side):
        mass = mass + part[0:nx]
    mass = jnp.sum(jnp.sum(mass, axis=0, keepdims=True), axis=1, keepdims=True)
    shift_all = jnp.broadcast_to(target[0] - mass / cells, (nx, width))
    is_fluid = fluid[...]

    def centre(v):
        return v[nx : 2 * nx, :width]

    def emit(k, value):
        mix[pl.ds(k, nx, stride=KROWS), :] = value

    change = [s - k for s, k in zip(state, kinetic)]
    for k in range(5):
        emit(k, centre(change[k]) * is_fluid)
        for d in range(3):
            emit(5 + 10 * d + k, centre(shift(change[k], d, -1)) * is_fluid)
            emit(10 + 10 * d + k, centre(shift(change[k], d, 1)) * is_fluid)
        emit(35 + k, centre(state[k]) * is_fluid)
    emit(40, shift_all * is_fluid)
    emit(41, heat[...] * (1.0 - is_fluid))
    for k in range(42, KROWS):
        emit(k, jnp.zeros((nx, width), f32))
    for k in range(5):
        value = centre(state[k])
        state_out[k] = value + shift_all if k == 0 else value


def macro(target, own, side, left, left_side, right, right_side, far, fluid, heat, cells, nz):
    nx, width = fluid.shape
    vmem = pl.BlockSpec(memory_space=pltpu.VMEM)
    return pl.pallas_call(
        functools.partial(macro_kernel, cells=cells, nz=nz, last=False),
        in_specs=[pl.BlockSpec(memory_space=pltpu.SMEM)] + [vmem] * 9,
        out_shape=[
            jax.ShapeDtypeStruct((KROWS * nx, width), f32),
            jax.ShapeDtypeStruct((5, nx, width), f32),
        ],
        name="macro",
    )(target, own, side, left, left_side, right, right_side, far, fluid, heat)


def update_kernel(g, mix, wmat, proj, coef, *outs, last):
    nx, ny, nz, nv = g.shape
    h = outs[0]
    half = nv // 2
    for x in range(nx):
        columns = mix[x * KROWS : (x + 1) * KROWS, :].T
        high, low = split(columns)
        lhs = jnp.concatenate([high, low, high], axis=1)
        add = dot(lhs, wmat[...], ((1,), (0,)))
        plane = g[x].reshape(ny * nz, nv) + add
        h[x] = plane.reshape(ny, nz, nv)
        if not last:
            mom, ysend, xup, xdown = outs[1:]
            out = local_moments(proj[...], plane)
            mom[pl.ds(x, MOMENTS, stride=nx), :] = out[:MOMENTS]
            ysend[x] = jnp.where(coef[4:5, :] > 0.0, plane[(ny - 1) * nz :], plane[:nz])
            if x == nx - 1:
                xup[...] = h[x, :, :, :half]
            if x == 0:
                xdown[...] = h[x, :, :, half:]


def update(g, mix, wmat, proj, coef, last):
    nx, ny, nz, nv = g.shape
    shapes = [jax.ShapeDtypeStruct(g.shape, f32)]
    if not last:
        shapes += [
            jax.ShapeDtypeStruct((MOMENTS * nx, ny * nz), f32),
            jax.ShapeDtypeStruct((nx, nz, nv), f32),
            jax.ShapeDtypeStruct((ny, nz, nv // 2), f32),
            jax.ShapeDtypeStruct((ny, nz, nv // 2), f32),
        ]
    return pl.pallas_call(
        functools.partial(update_kernel, last=last),
        out_shape=shapes,
        name="update",
    )(g, mix, wmat, proj, coef)


def ring(value, axis, step):
    count = lax.axis_size(axis)
    return lax.ppermute(value, axis, [(i, (i + step) % count) for i in range(count)])


def on_device(initial, velocity, weights, wall, wall_temp, mass_target):
    nx, ny, nz, nv = initial.shape
    width = ny * nz
    n_tx, n_ty, n_vel = (lax.axis_size(a) for a in ("tx", "ty", "vel"))
    if n_ty != 2 or n_tx < 3 or nx <= MACRO_STEPS or width != LANES or n_vel & (n_vel - 1):
        raise ValueError("unsupported sizes")
    cells = float(nx * width * n_tx * n_ty)
    top = n_vel // 2

    def plane_pair(value, flip_y, flip_v):
        pairs = []
        for y in range(n_ty):
            for v in range(n_vel):
                pairs.append((y * n_vel + v, (y ^ flip_y) * n_vel + (v ^ flip_v)))
        return lax.ppermute(value, ("ty", "vel"), pairs)

    fluid = jnp.where(wall == 1, 0.0, 1.0).astype(f32)
    fluid_rows = fluid.reshape(nx, width)
    heat = wall_temp.reshape(nx, width)
    fluid_cells = jnp.broadcast_to(fluid[..., None], (nx, ny, nz, LANES))
    target = mass_target[None]
    mom, proj, wmat, coef, ysend, xup, xdown = prepare(initial, velocity, weights, float(nv * n_vel))
    h = initial
    for iteration in range(ITERS):
        last = iteration == ITERS - 1
        bit = 1
        while bit < top:
            mom = mom + plane_pair(mom, 0, bit)
            bit *= 2
        own = mom + plane_pair(mom, 0, top)
        side = plane_pair(mom, 1, 0) + plane_pair(mom, 1, top)
        left, left_side = ring(own, "tx", 1), ring(side, "tx", 1)
        right, right_side = ring(own, "tx", -1), ring(side, "tx", -1)
        sums = own[0:nx] + side[0:nx]
        far = sum([ring(sums, "tx", d) for d in range(2, n_tx - 1)], jnp.zeros_like(sums))
        yhalo = ring(ysend, "ty", 1)
        xbefore, xafter = ring(xup, "tx", 1), ring(xdown, "tx", -1)
        g = stream(h, yhalo, xbefore, xafter, coef, fluid_cells)
        mix, state = macro(target, own, side, left, left_side, right, right_side, far, fluid_rows, heat, cells, nz)
        outs = update(g, mix, wmat, proj, coef, last)
        h = outs[0]
        if not last:
            mom, ysend, xup, xdown = outs[1:]
    return h, state.reshape(5, nx, ny, nz)


def solution(mesh):
    placed = (
        P("tx", "ty", None, "vel"),
        P(None, "vel"),
        P("vel"),
        P("tx", "ty", None),
        P("tx", "ty", None),
        P(),
    )
    return jax.shard_map(
        on_device,
        mesh=mesh,
        in_specs=placed,
        out_specs=(P("tx", "ty", None, "vel"), P(None, "tx", "ty", None)),
        check_vma=False,
    )
```

```python
import functools

import jax
import jax.numpy as jnp
from jax import lax
from jax.experimental import pallas as pl
from jax.experimental.pallas import tpu as pltpu
from jax.sharding import PartitionSpec as P


ITERS = 3
MACRO_STEPS = 4

STEP_TIME = 0.1
COLLISION = 1.0
MACRO_TIME = 0.1
VISCOSITY = 1.0
CONDUCTION = 1.0

LANES = 128
MOMENTS = 14
PROWS = 16
KROWS = 48
f32 = jnp.float32
bf16 = jnp.bfloat16


def split(value):
    high = value.astype(bf16)
    return high, (value - high.astype(f32)).astype(bf16)


def dot(a, b, contract):
    return lax.dot_general(a, b, (contract, ((), ())), preferred_element_type=f32)


def local_moments(proj, plane):
    high, low = split(plane)
    both = dot(proj, high, ((1,), (1,)))
    return both[:PROWS] + both[PROWS:] + dot(proj[:PROWS], low, ((1,), (1,)))


def prepare_kernel(vel, wgt, h, mom, proj, wmat, coef, ysend, xup, xdown, rows, *, total):
    x = pl.program_id(0)
    planes = pl.num_programs(0)
    vx, vy, vz = vel[0:1, :], vel[1:2, :], vel[2:3, :]

    @pl.when(x == 0)
    def _():
        speed = vx * vx + vy * vy + vz * vz
        scale = wgt[...] / total
        one = jnp.ones_like(speed)
        zero = jnp.zeros_like(speed)
        table = [
            one,
            vx,
            vy,
            vz,
            2.0 / 3.0 * speed - 1.0,
            2.0 * (vx * vx - speed / 3.0),
            2.0 * (vy * vy - speed / 3.0),
            2.0 * (vz * vz - speed / 3.0),
            2.0 * vx * vy,
            2.0 * vx * vz,
            2.0 * vy * vz,
            vx * (speed - 2.5),
            vy * (speed - 2.5),
            vz * (speed - 2.5),
        ]
        for k, row in enumerate(table):
            rows[k : k + 1, :] = row * scale
        for k in range(MOMENTS, PROWS):
            rows[k : k + 1, :] = zero
        high, low = split(rows[0:PROWS, :])
        proj[0:PROWS, :] = high
        proj[PROWS : 2 * PROWS, :] = low
        along_x, along_y, along_z = (STEP_TIME * jnp.abs(v) for v in (vx, vy, vz))
        centre = (1.0 - STEP_TIME * COLLISION) - (along_x + along_y + along_z)
        for k, row in enumerate([centre, along_x, along_y, along_z, vy, vz, zero, zero]):
            coef[k : k + 1, :] = row
        basis = [one, 2.0 * vx, 2.0 * vy, 2.0 * vz, speed - 1.5]
        parts = [
            centre,
            jnp.where(vx > 0.0, along_x, 0.0),
            jnp.where(vx > 0.0, 0.0, along_x),
            jnp.where(vy > 0.0, along_y, 0.0),
            jnp.where(vy > 0.0, 0.0, along_y),
            jnp.where(vz > 0.0, along_z, 0.0),
            jnp.where(vz > 0.0, 0.0, along_z),
            STEP_TIME * COLLISION * one,
        ]
        for i, part in enumerate(parts):
            for k, row in enumerate(basis):
                rows[5 * i + k : 5 * i + k + 1, :] = part * row
        rows[40:41, :] = one
        rows[41:42, :] = basis[4]
        for k in range(42, KROWS):
            rows[k : k + 1, :] = zero
        high, low = split(rows[...])
        wmat[0:KROWS, :] = high
        wmat[KROWS : 2 * KROWS, :] = high
        wmat[2 * KROWS : 3 * KROWS, :] = low

    _, ny, nz, nv = h.shape
    plane = h[0].reshape(ny * nz, nv)
    out = local_moments(proj[...], plane)
    mom[pl.ds(x, MOMENTS, stride=planes), :] = out[:MOMENTS]
    ysend[0] = jnp.where(vy > 0.0, plane[(ny - 1) * nz :], plane[:nz])

    @pl.when(x == planes - 1)
    def _():
        xup[...] = h[0, :, :, : nv // 2]

    @pl.when(x == 0)
    def _():
        xdown[...] = h[0, :, :, nv // 2 :]


def prepare(initial, velocity, weights, total):
    nx, ny, nz, nv = initial.shape
    whole = lambda *shape: pl.BlockSpec(shape, lambda x: (0,) * len(shape))
    return pl.pallas_call(
        functools.partial(prepare_kernel, total=total),
        grid=(nx,),
        in_specs=[whole(3, nv), whole(1, nv), pl.BlockSpec((1, ny, nz, nv), lambda x: (x, 0, 0, 0))],
        out_specs=[
            whole(MOMENTS * nx, ny * nz),
            whole(2 * PROWS, nv),
            whole(3 * KROWS, nv),
            whole(8, nv),
            pl.BlockSpec((1, nz, nv), lambda x: (x, 0, 0)),
            whole(ny, nz, nv // 2),
            whole(ny, nz, nv // 2),
        ],
        out_shape=[
            jax.ShapeDtypeStruct((MOMENTS * nx, ny * nz), f32),
            jax.ShapeDtypeStruct((2 * PROWS, nv), bf16),
            jax.ShapeDtypeStruct((3 * KROWS, nv), bf16),
            jax.ShapeDtypeStruct((8, nv), f32),
            jax.ShapeDtypeStruct((nx, nz, nv), f32),
            jax.ShapeDtypeStruct((ny, nz, nv // 2), f32),
            jax.ShapeDtypeStruct((ny, nz, nv // 2), f32),
        ],
        scratch_shapes=[pltpu.VMEM((KROWS, nv), f32)],
        name="prepare",
        compiler_params=pltpu.CompilerParams(vmem_limit_bytes=8 << 20),
    )(velocity, weights[None], initial)


def y_direction(lanes, nv):
    quarters = {(lanes.start * 4) // nv, ((lanes.stop - 1) * 4) // nv}
    return {q % 2 == 0 for q in quarters}


def stream_kernel(h, coef, fluid, g):
    nx, ny, nz, nv = h.shape
    tiles = nv // LANES
    for j in range(tiles):
        lanes = slice(j * LANES, (j + 1) * LANES)
        forward_x = j < tiles // 2
        row = lambda k: jnp.broadcast_to(coef[k : k + 1, lanes], (nz, LANES))
        centre, along_x, along_y, along_z = (row(k) for k in range(4))
        up_z = row(5) > 0.0
        up_y = row(4) > 0.0
        signs = y_direction(lanes, nv)
        zero = jnp.zeros((nz, LANES), f32)
        for x in range(nx):
            for y in range(ny):
                c = h[x, y, :, lanes]
                beside = x - 1 if forward_x else x + 1
                ux = h[beside, y, :, lanes] if 0 <= beside < nx else None
                before = h[x, y - 1, :, lanes] if y > 0 else None
                after = h[x, y + 1, :, lanes] if y < ny - 1 else None
                if signs == {True}:
                    uy = before
                elif signs == {False}:
                    uy = after
                else:
                    uy = jnp.where(up_y, zero if before is None else before, zero if after is None else after)
                uz = jnp.where(up_z, pltpu.roll(c, 1, 0), pltpu.roll(c, nz - 1, 0))
                out = centre * c + along_z * uz
                if ux is not None:
                    out = out + along_x * ux
                if uy is not None:
                    out = out + along_y * uy
                g[x, y, :, lanes] = out * fluid[x, y]


def stream(h, coef, fluid):
    return pl.pallas_call(
        stream_kernel,
        out_shape=jax.ShapeDtypeStruct(h.shape, f32),
        name="stream",
        compiler_params=pltpu.CompilerParams(vmem_limit_bytes=12 << 20),
    )(h, coef, fluid)


def join_kernel(mom, across, beside, corner, both, mass):
    rows = mom.shape[0]
    nx = mass.shape[0]
    own = mom[...] + across[...]
    side = beside[...] + corner[...]
    both[0:rows, :] = own
    both[rows:, :] = side
    mass[...] = own[0:nx] + side[0:nx]


def join(mom, across, beside, corner, nx):
    rows, width = mom.shape
    return pl.pallas_call(
        join_kernel,
        out_shape=[
            jax.ShapeDtypeStruct((2 * rows, width), f32),
            jax.ShapeDtypeStruct((nx, width), f32),
        ],
        name="join",
        compiler_params=pltpu.CompilerParams(vmem_limit_bytes=4 << 20),
    )(mom, across, beside, corner)


def macro_kernel(mid, left, right, fluid, heat, mix, state_out, mass_out, *, nz):
    nx, width = fluid.shape

    def field(k):
        halves = []
        for start in (k * nx, (MOMENTS + k) * nx):
            part = slice(start, start + nx)
            halves.append(jnp.concatenate([left[part], mid[part], right[part]], axis=0))
        return jnp.concatenate(halves, axis=1)

    rows, lanes = 3 * nx, 2 * width
    depth = lax.broadcasted_iota(jnp.int32, (rows, lanes), 1) % nz
    first, final = depth == 0, depth == nz - 1

    def shift(v, direction, offset):
        if direction == 0:
            return pltpu.roll(v, 1 if offset < 0 else rows - 1, 0)
        if direction == 1:
            return pltpu.roll(v, nz if offset < 0 else lanes - nz, 1)
        if offset < 0:
            return jnp.where(first, pltpu.roll(v, lanes - nz + 1, 1), pltpu.roll(v, 1, 1))
        return jnp.where(final, pltpu.roll(v, nz - 1, 1), pltpu.roll(v, lanes - 1, 1))

    def around(v, directions=(0, 1, 2)):
        return {d: (shift(v, d, 1), shift(v, d, -1)) for d in directions}

    def grad(pair):
        return (pair[0] - pair[1]) * 0.5

    def laplace(v, near):
        total = (near[0][0] + near[0][1]) + (near[1][0] + near[1][1]) + (near[2][0] + near[2][1])
        return total - 6.0 * v

    def slope(v, d):
        return grad(around(v, (d,))[d])

    state = [field(k) for k in range(5)]
    kinetic = state
    near = [None] + [around(state[k]) for k in range(1, 5)]
    stress = [field(5 + k) for k in range(9)]
    sums = [
        slope(stress[0], 0) + slope(stress[3], 1) + slope(stress[4], 2),
        slope(stress[3], 0) + slope(stress[1], 1) + slope(stress[5], 2),
        slope(stress[4], 0) + slope(stress[5], 1) + slope(stress[2], 2),
    ]
    flow = slope(stress[6], 0) + slope(stress[7], 1) + slope(stress[8], 2)
    sources = [-0.5 * (sums[i] + VISCOSITY * laplace(state[1 + i], near[1 + i])) for i in range(3)]
    sources.append(-(2.0 / 3.0) * (flow + CONDUCTION * laplace(state[4], near[4])))
    for step in range(MACRO_STEPS):
        if step:
            near = [None] + [around(state[k]) for k in range(1, 5)]
        near[0] = around(state[0])
        div = grad(near[1][0]) + grad(near[2][1]) + grad(near[3][2])
        rates = [-div]
        for i in range(3):
            rates.append(
                -0.5 * (grad(near[0][i]) + grad(near[4][i]))
                + 0.5 * VISCOSITY * laplace(state[1 + i], near[1 + i])
                + sources[i]
            )
        rates.append(-(2.0 / 3.0) * div + 2.0 / 3.0 * CONDUCTION * laplace(state[4], near[4]) + sources[3])
        state = [s + MACRO_TIME * r for s, r in zip(state, rates)]

    mass = None
    for part in (mid, left, right):
        for start in (0, MOMENTS * nx):
            mass = part[start : start + nx] if mass is None else mass + part[start : start + nx]
    mass_out[...] = mass
    is_fluid = fluid[...]

    def centre(v):
        return v[nx : 2 * nx, :width]

    def emit(k, value):
        mix[pl.ds(k, nx, stride=KROWS), :] = value

    change = [s - k for s, k in zip(state, kinetic)]
    for k in range(5):
        emit(k, centre(change[k]) * is_fluid)
        for d in range(3):
            emit(5 + 10 * d + k, centre(shift(change[k], d, -1)) * is_fluid)
            emit(10 + 10 * d + k, centre(shift(change[k], d, 1)) * is_fluid)
        emit(35 + k, centre(state[k]) * is_fluid)
    emit(40, is_fluid)
    emit(41, heat[...] * (1.0 - is_fluid))
    for k in range(42, KROWS):
        emit(k, jnp.zeros((nx, width), f32))
    for k in range(5):
        state_out[k] = centre(state[k])


def macro(mid, left, right, fluid, heat, nz):
    nx, width = fluid.shape
    return pl.pallas_call(
        functools.partial(macro_kernel, nz=nz),
        out_shape=[
            jax.ShapeDtypeStruct((KROWS * nx, width), f32),
            jax.ShapeDtypeStruct((5, nx, width), f32),
            jax.ShapeDtypeStruct((nx, width), f32),
        ],
        name="macro",
        compiler_params=pltpu.CompilerParams(vmem_limit_bytes=8 << 20),
    )(mid, left, right, fluid, heat)


def update_kernel(target, g, mix, wmat, proj, coef, fluid, yhalo, xbefore, xafter, mass, far, *refs, last, cells):
    nx, ny, nz, nv = g.shape
    half = nv // 2
    if last:
        state, h, fields = refs
    else:
        h, mom, ysend, xup, xdown = refs
    total = mass[...] + far[...]
    total = jnp.sum(jnp.sum(total, axis=0, keepdims=True), axis=1, keepdims=True)
    offset = target[0] - total / cells
    is_offset = lax.broadcasted_iota(jnp.int32, (KROWS, ny * nz), 0) == 40
    scale = jnp.where(is_offset, jnp.broadcast_to(offset, (KROWS, ny * nz)), 1.0)
    if last:
        for k in range(5):
            value = state[k] + jnp.broadcast_to(offset, (nx, ny * nz)) if k == 0 else state[k]
            for y in range(ny):
                fields[pl.ds(k * nx * ny + y, nx, stride=ny), :] = value[:, y * nz : (y + 1) * nz]
    along_x, along_y = coef[1:2, :], coef[2:3, :]
    upward = coef[4:5, :] > 0.0
    first_y = jnp.where(upward, along_y, 0.0)
    final_y = jnp.where(upward, 0.0, along_y)
    for x in range(nx):
        columns = (mix[x * KROWS : (x + 1) * KROWS, :] * scale).T
        high, low = split(columns)
        lhs = jnp.concatenate([high, low, high], axis=1)
        add = dot(lhs, wmat[...], ((1,), (0,)))
        pieces = []
        for y in range(ny):
            piece = g[x, y] + add[y * nz : (y + 1) * nz]
            outer = None
            if y == 0:
                outer = first_y * yhalo[x]
            if y == ny - 1:
                outer = final_y * yhalo[x]
            if x == 0:
                edge = jnp.concatenate([along_x[:, :half] * xbefore[y], jnp.zeros((nz, half), f32)], axis=1)
                outer = edge if outer is None else outer + edge
            if x == nx - 1:
                edge = jnp.concatenate([jnp.zeros((nz, half), f32), along_x[:, half:] * xafter[y]], axis=1)
                outer = edge if outer is None else outer + edge
            if outer is not None:
                piece = piece + outer * jnp.concatenate([fluid[x, y]] * (nv // LANES), axis=1)
            pieces.append(piece)
        plane = jnp.concatenate(pieces, axis=0)
        h[x] = plane.reshape(ny, nz, nv)
        if not last:
            out = local_moments(proj[...], plane)
            mom[pl.ds(x, MOMENTS, stride=nx), :] = out[:MOMENTS]
            ysend[x] = jnp.where(upward, plane[(ny - 1) * nz :], plane[:nz])
            if x == nx - 1:
                xup[...] = h[x, :, :, :half]
            if x == 0:
                xdown[...] = h[x, :, :, half:]


def update(target, g, mix, wmat, proj, coef, fluid, halos, mass, far, state, cells):
    nx, ny, nz, nv = g.shape
    last = state is not None
    shapes = [jax.ShapeDtypeStruct(g.shape, f32)]
    if last:
        shapes.append(jax.ShapeDtypeStruct((5 * nx * ny, nz), f32))
    else:
        shapes += [
            jax.ShapeDtypeStruct((MOMENTS * nx, ny * nz), f32),
            jax.ShapeDtypeStruct((nx, nz, nv), f32),
            jax.ShapeDtypeStruct((ny, nz, nv // 2), f32),
            jax.ShapeDtypeStruct((ny, nz, nv // 2), f32),
        ]
    operands = [target, g, mix, wmat, proj, coef, fluid, *halos, mass, far]
    if last:
        operands.append(state)
    vmem = pl.BlockSpec(memory_space=pltpu.VMEM)
    return pl.pallas_call(
        functools.partial(update_kernel, last=last, cells=cells),
        in_specs=[pl.BlockSpec(memory_space=pltpu.SMEM)] + [vmem] * (len(operands) - 1),
        out_shape=shapes,
        name="update",
        compiler_params=pltpu.CompilerParams(vmem_limit_bytes=14 << 20),
    )(*operands)


def ring(value, axis, step):
    count = lax.axis_size(axis)
    return lax.ppermute(value, axis, [(i, (i + step) % count) for i in range(count)])


def on_device(initial, velocity, weights, wall, wall_temp, mass_target):
    nx, ny, nz, nv = initial.shape
    width = ny * nz
    n_tx, n_ty, n_vel = (lax.axis_size(a) for a in ("tx", "ty", "vel"))
    if n_ty != 2 or n_tx < 3 or nx <= MACRO_STEPS or width != LANES or n_vel & (n_vel - 1):
        raise ValueError("unsupported sizes")
    cells = float(nx * width * n_tx * n_ty)
    top = n_vel // 2

    def plane_pair(value, flip_y, flip_v):
        pairs = []
        for y in range(n_ty):
            for v in range(n_vel):
                pairs.append((y * n_vel + v, (y ^ flip_y) * n_vel + (v ^ flip_v)))
        return lax.ppermute(value, ("ty", "vel"), pairs)

    fluid = jnp.where(wall == 1, 0.0, 1.0).astype(f32)
    fluid_rows = fluid.reshape(nx, width)
    heat = wall_temp.reshape(nx, width)
    fluid_cells = jnp.broadcast_to(fluid[..., None], (nx, ny, nz, LANES))
    target = mass_target[None]
    mom, proj, wmat, coef, ysend, xup, xdown = prepare(initial, velocity, weights, float(nv * n_vel))
    h = initial
    for iteration in range(ITERS):
        last = iteration == ITERS - 1
        bit = 1
        while bit < top:
            mom = mom + plane_pair(mom, 0, bit)
            bit *= 2
        across = plane_pair(mom, 0, top)
        beside = plane_pair(mom, 1, 0)
        corner = plane_pair(mom, 1, top)
        yhalo = ring(ysend, "ty", 1)
        xbefore = ring(xup, "tx", 1)
        xafter = ring(xdown, "tx", -1)
        both, sums = join(mom, across, beside, corner, nx)
        left = ring(both, "tx", 1)
        right = ring(both, "tx", -1)
        far = None
        for d in range(2, n_tx - 1):
            part = ring(sums, "tx", d)
            far = part if far is None else far + part
        if far is None:
            far = jnp.zeros_like(sums)
        g = stream(h, coef, fluid_cells)
        mix, state, mass = macro(both, left, right, fluid_rows, heat, nz)
        halos = (yhalo, xbefore, xafter)
        outs = update(target, g, mix, wmat, proj, coef, fluid_cells, halos, mass, far, state if last else None, cells)
        h = outs[0]
        if not last:
            mom, ysend, xup, xdown = outs[1:]
    return h, outs[1].reshape(5, nx, ny, nz)


def solution(mesh):
    placed = (
        P("tx", "ty", None, "vel"),
        P(None, "vel"),
        P("vel"),
        P("tx", "ty", None),
        P("tx", "ty", None),
        P(),
    )
    return jax.shard_map(
        on_device,
        mesh=mesh,
        in_specs=placed,
        out_specs=(P("tx", "ty", None, "vel"), P(None, "tx", "ty", None)),
        check_vma=False,
    )
```

```python
import functools

import jax
import jax.numpy as jnp
from jax import lax
from jax.experimental import pallas as pl
from jax.experimental.pallas import tpu as pltpu
from jax.sharding import PartitionSpec as P


ITERS = 3
MACRO_STEPS = 4

STEP_TIME = 0.1
COLLISION = 1.0
MACRO_TIME = 0.1
VISCOSITY = 1.0
CONDUCTION = 1.0

LANES = 128
MOMENTS = 14
PROWS = 16
KROWS = 48
f32 = jnp.float32
bf16 = jnp.bfloat16


def split(value):
    high = value.astype(bf16)
    return high, (value - high.astype(f32)).astype(bf16)


def dot(a, b, contract):
    return lax.dot_general(a, b, (contract, ((), ())), preferred_element_type=f32)


def local_moments(proj, plane):
    high, low = split(plane)
    both = dot(proj, high, ((1,), (1,)))
    return both[:PROWS] + both[PROWS:] + dot(proj[:PROWS], low, ((1,), (1,)))


def prepare_kernel(
    vel_far, wgt_far, target_far, source, h, mom, proj, wmat, coef, ysend, xup, xdown, goal, rows, vel, wgt, target, arrived, *, total
):
    planes, ny, nz, nv = source.shape
    order = [planes - 1, *range(planes - 1)]
    copies = [pltpu.make_async_copy(source.at[x], h.at[x], arrived.at[x]) for x in range(planes)]
    small = [
        pltpu.make_async_copy(far, near, arrived.at[planes + i])
        for i, (far, near) in enumerate([(vel_far, vel), (wgt_far, wgt), (target_far, target)])
    ]
    for copy in small:
        copy.start()
    for x in order:
        copies[x].start()
    for copy in small:
        copy.wait()
    goal[...] = jnp.full(goal.shape, target[0], f32)
    vx, vy, vz = vel[0:1, :], vel[1:2, :], vel[2:3, :]

    speed = vx * vx + vy * vy + vz * vz
    scale = wgt[...].reshape(1, nv) / total
    one = jnp.ones_like(speed)
    zero = jnp.zeros_like(speed)
    table = [
        one,
        vx,
        vy,
        vz,
        2.0 / 3.0 * speed - 1.0,
        2.0 * (vx * vx - speed / 3.0),
        2.0 * (vy * vy - speed / 3.0),
        2.0 * (vz * vz - speed / 3.0),
        2.0 * vx * vy,
        2.0 * vx * vz,
        2.0 * vy * vz,
        vx * (speed - 2.5),
        vy * (speed - 2.5),
        vz * (speed - 2.5),
    ]
    for k, row in enumerate(table):
        rows[k : k + 1, :] = row * scale
    for k in range(MOMENTS, PROWS):
        rows[k : k + 1, :] = zero
    high, low = split(rows[0:PROWS, :])
    proj[0:PROWS, :] = high
    proj[PROWS : 2 * PROWS, :] = low
    along_x, along_y, along_z = (STEP_TIME * jnp.abs(v) for v in (vx, vy, vz))
    centre = (1.0 - STEP_TIME * COLLISION) - (along_x + along_y + along_z)
    for k, row in enumerate([centre, along_x, along_y, along_z, vy, vz, zero, zero]):
        coef[k : k + 1, :] = row
    basis = [one, 2.0 * vx, 2.0 * vy, 2.0 * vz, speed - 1.5]
    parts = [
        centre,
        jnp.where(vx > 0.0, along_x, 0.0),
        jnp.where(vx > 0.0, 0.0, along_x),
        jnp.where(vy > 0.0, along_y, 0.0),
        jnp.where(vy > 0.0, 0.0, along_y),
        jnp.where(vz > 0.0, along_z, 0.0),
        jnp.where(vz > 0.0, 0.0, along_z),
        STEP_TIME * COLLISION * one,
    ]
    for i, part in enumerate(parts):
        for k, row in enumerate(basis):
            rows[5 * i + k : 5 * i + k + 1, :] = part * row
    rows[40:41, :] = one
    rows[41:42, :] = basis[4]
    for k in range(42, KROWS):
        rows[k : k + 1, :] = zero
    high, low = split(rows[...])
    wmat[0:KROWS, :] = high
    wmat[KROWS : 2 * KROWS, :] = high
    wmat[2 * KROWS : 3 * KROWS, :] = low

    for x in order:
        copies[x].wait()
        plane = h[x].reshape(ny * nz, nv)
        out = local_moments(proj[...], plane)
        mom[pl.ds(x, MOMENTS, stride=planes), :] = out[:MOMENTS]
        ysend[x] = jnp.where(vy > 0.0, plane[(ny - 1) * nz :], plane[:nz])
        if x == planes - 1:
            xup[...] = h[x, :, :, : nv // 2]
        if x == 0:
            xdown[...] = h[x, :, :, nv // 2 :]


def prepare(initial, velocity, weights, target, total):
    nx, ny, nz, nv = initial.shape
    return pl.pallas_call(
        functools.partial(prepare_kernel, total=total),
        in_specs=[pl.BlockSpec(memory_space=pltpu.HBM)] * 4,
        out_shape=[
            jax.ShapeDtypeStruct(initial.shape, f32),
            jax.ShapeDtypeStruct((MOMENTS * nx, ny * nz), f32),
            jax.ShapeDtypeStruct((2 * PROWS, nv), bf16),
            jax.ShapeDtypeStruct((3 * KROWS, nv), bf16),
            jax.ShapeDtypeStruct((8, nv), f32),
            jax.ShapeDtypeStruct((nx, nz, nv), f32),
            jax.ShapeDtypeStruct((ny, nz, nv // 2), f32),
            jax.ShapeDtypeStruct((ny, nz, nv // 2), f32),
            jax.ShapeDtypeStruct((8, LANES), f32),
        ],
        scratch_shapes=[
            pltpu.VMEM((KROWS, nv), f32),
            pltpu.VMEM(velocity.shape, f32),
            pltpu.VMEM(weights.shape, f32),
            pltpu.SMEM((1,), f32),
            pltpu.SemaphoreType.DMA((nx + 3,)),
        ],
        name="prepare",
        compiler_params=pltpu.CompilerParams(vmem_limit_bytes=12 << 20),
    )(*(pltpu.with_memory_space_constraint(v, pltpu.HBM) for v in (velocity, weights)), target, pltpu.with_memory_space_constraint(initial, pltpu.HBM))


def walls_kernel(wall, wall_temp, rows, heat, cells):
    nx, ny, nz = wall.shape
    square = (nz, nz)
    same = lax.broadcasted_iota(jnp.int32, square, 0) == lax.broadcasted_iota(jnp.int32, square, 1)
    for x in range(nx):
        open_cells = jnp.where(wall[x] == 1, 0.0, 1.0)
        temps = wall_temp[x]
        for y in range(ny):
            part = slice(y * nz, (y + 1) * nz)
            rows[x : x + 1, part] = open_cells[y : y + 1]
            heat[x : x + 1, part] = temps[y : y + 1]
            spread = jnp.where(same, jnp.broadcast_to(open_cells[y : y + 1], square), 0.0)
            cells[x, y] = jnp.broadcast_to(jnp.sum(spread, axis=1, keepdims=True), (nz, LANES))


def walls(wall, wall_temp):
    nx, ny, nz = wall.shape
    return pl.pallas_call(
        walls_kernel,
        out_shape=[
            jax.ShapeDtypeStruct((nx, ny * nz), f32),
            jax.ShapeDtypeStruct((nx, ny * nz), f32),
            jax.ShapeDtypeStruct((nx, ny, nz, LANES), f32),
        ],
        name="walls",
        compiler_params=pltpu.CompilerParams(vmem_limit_bytes=6 << 20),
    )(wall, wall_temp)


def y_direction(lanes, nv):
    quarters = {(lanes.start * 4) // nv, ((lanes.stop - 1) * 4) // nv}
    return {q % 2 == 0 for q in quarters}


def stream_kernel(h, coef, fluid, g):
    nx, ny, nz, nv = h.shape
    tiles = nv // LANES
    for j in range(tiles):
        lanes = slice(j * LANES, (j + 1) * LANES)
        forward_x = j < tiles // 2
        row = lambda k: jnp.broadcast_to(coef[k : k + 1, lanes], (nz, LANES))
        centre, along_x, along_y, along_z = (row(k) for k in range(4))
        up_z = row(5) > 0.0
        up_y = row(4) > 0.0
        signs = y_direction(lanes, nv)
        zero = jnp.zeros((nz, LANES), f32)
        for x in range(nx):
            for y in range(ny):
                c = h[x, y, :, lanes]
                beside = x - 1 if forward_x else x + 1
                ux = h[beside, y, :, lanes] if 0 <= beside < nx else None
                before = h[x, y - 1, :, lanes] if y > 0 else None
                after = h[x, y + 1, :, lanes] if y < ny - 1 else None
                if signs == {True}:
                    uy = before
                elif signs == {False}:
                    uy = after
                else:
                    uy = jnp.where(up_y, zero if before is None else before, zero if after is None else after)
                uz = jnp.where(up_z, pltpu.roll(c, 1, 0), pltpu.roll(c, nz - 1, 0))
                out = centre * c + along_z * uz
                if ux is not None:
                    out = out + along_x * ux
                if uy is not None:
                    out = out + along_y * uy
                g[x, y, :, lanes] = out * fluid[x, y]


def stream(h, coef, fluid):
    return pl.pallas_call(
        stream_kernel,
        out_shape=jax.ShapeDtypeStruct(h.shape, f32),
        name="stream",
        compiler_params=pltpu.CompilerParams(vmem_limit_bytes=12 << 20),
    )(h, coef, fluid)


def join_kernel(mom, across, beside, corner, both, mass):
    rows = mom.shape[0]
    nx = mass.shape[0]
    own = mom[...] + across[...]
    side = beside[...] + corner[...]
    both[0:rows, :] = own
    both[rows:, :] = side
    mass[...] = own[0:nx] + side[0:nx]


def join(mom, across, beside, corner, nx):
    rows, width = mom.shape
    return pl.pallas_call(
        join_kernel,
        out_shape=[
            jax.ShapeDtypeStruct((2 * rows, width), f32),
            jax.ShapeDtypeStruct((nx, width), f32),
        ],
        name="join",
        compiler_params=pltpu.CompilerParams(vmem_limit_bytes=4 << 20),
    )(mom, across, beside, corner)


def macro_kernel(mid, left, right, fluid, heat, mix, state_out, mass_out, *, nz):
    nx, width = fluid.shape

    def field(k):
        halves = []
        for start in (k * nx, (MOMENTS + k) * nx):
            part = slice(start, start + nx)
            halves.append(jnp.concatenate([left[part], mid[part], right[part]], axis=0))
        return jnp.concatenate(halves, axis=1)

    rows, lanes = 3 * nx, 2 * width
    depth = lax.broadcasted_iota(jnp.int32, (rows, lanes), 1) % nz
    first, final = depth == 0, depth == nz - 1

    def shift(v, direction, offset):
        if direction == 0:
            return pltpu.roll(v, 1 if offset < 0 else rows - 1, 0)
        if direction == 1:
            return pltpu.roll(v, nz if offset < 0 else lanes - nz, 1)
        if offset < 0:
            return jnp.where(first, pltpu.roll(v, lanes - nz + 1, 1), pltpu.roll(v, 1, 1))
        return jnp.where(final, pltpu.roll(v, nz - 1, 1), pltpu.roll(v, lanes - 1, 1))

    def around(v, directions=(0, 1, 2)):
        return {d: (shift(v, d, 1), shift(v, d, -1)) for d in directions}

    def grad(pair):
        return (pair[0] - pair[1]) * 0.5

    def laplace(v, near):
        total = (near[0][0] + near[0][1]) + (near[1][0] + near[1][1]) + (near[2][0] + near[2][1])
        return total - 6.0 * v

    def slope(v, d):
        return grad(around(v, (d,))[d])

    state = [field(k) for k in range(5)]
    kinetic = state
    near = [None] + [around(state[k]) for k in range(1, 5)]
    stress = [field(5 + k) for k in range(9)]
    sums = [
        slope(stress[0], 0) + slope(stress[3], 1) + slope(stress[4], 2),
        slope(stress[3], 0) + slope(stress[1], 1) + slope(stress[5], 2),
        slope(stress[4], 0) + slope(stress[5], 1) + slope(stress[2], 2),
    ]
    flow = slope(stress[6], 0) + slope(stress[7], 1) + slope(stress[8], 2)
    sources = [-0.5 * (sums[i] + VISCOSITY * laplace(state[1 + i], near[1 + i])) for i in range(3)]
    sources.append(-(2.0 / 3.0) * (flow + CONDUCTION * laplace(state[4], near[4])))
    for step in range(MACRO_STEPS):
        if step:
            near = [None] + [around(state[k]) for k in range(1, 5)]
        near[0] = around(state[0])
        div = grad(near[1][0]) + grad(near[2][1]) + grad(near[3][2])
        rates = [-div]
        for i in range(3):
            rates.append(
                -0.5 * (grad(near[0][i]) + grad(near[4][i]))
                + 0.5 * VISCOSITY * laplace(state[1 + i], near[1 + i])
                + sources[i]
            )
        rates.append(-(2.0 / 3.0) * div + 2.0 / 3.0 * CONDUCTION * laplace(state[4], near[4]) + sources[3])
        state = [s + MACRO_TIME * r for s, r in zip(state, rates)]

    mass = None
    for part in (mid, left, right):
        for start in (0, MOMENTS * nx):
            mass = part[start : start + nx] if mass is None else mass + part[start : start + nx]
    mass_out[...] = mass
    is_fluid = fluid[...]

    def centre(v):
        return v[nx : 2 * nx, :width]

    def emit(k, value):
        mix[pl.ds(k, nx, stride=KROWS), :] = value

    change = [s - k for s, k in zip(state, kinetic)]
    for k in range(5):
        emit(k, centre(change[k]) * is_fluid)
        for d in range(3):
            emit(5 + 10 * d + k, centre(shift(change[k], d, -1)) * is_fluid)
            emit(10 + 10 * d + k, centre(shift(change[k], d, 1)) * is_fluid)
        emit(35 + k, centre(state[k]) * is_fluid)
    emit(40, is_fluid)
    emit(41, heat[...] * (1.0 - is_fluid))
    for k in range(42, KROWS):
        emit(k, jnp.zeros((nx, width), f32))
    for k in range(5):
        state_out[k] = centre(state[k])


def macro(mid, left, right, fluid, heat, nz):
    nx, width = fluid.shape
    return pl.pallas_call(
        functools.partial(macro_kernel, nz=nz),
        out_shape=[
            jax.ShapeDtypeStruct((KROWS * nx, width), f32),
            jax.ShapeDtypeStruct((5, nx, width), f32),
            jax.ShapeDtypeStruct((nx, width), f32),
        ],
        name="macro",
        compiler_params=pltpu.CompilerParams(vmem_limit_bytes=8 << 20),
    )(mid, left, right, fluid, heat)


def update_kernel(target, g, mix, wmat, proj, coef, fluid, yhalo, xbefore, xafter, mass, far, *refs, last, cells):
    nx, ny, nz, nv = g.shape
    half = nv // 2
    if last:
        state, result, fields, h, sent = refs
        copies = [pltpu.make_async_copy(h.at[x], result.at[x], sent.at[x]) for x in range(nx)]
    else:
        h, mom, ysend, xup, xdown = refs
    total = mass[...] + far[...]
    total = jnp.sum(jnp.sum(total, axis=0, keepdims=True), axis=1, keepdims=True)
    offset = target[0:1, 0:1] - total / cells
    is_offset = lax.broadcasted_iota(jnp.int32, (KROWS, ny * nz), 0) == 40
    scale = jnp.where(is_offset, jnp.broadcast_to(offset, (KROWS, ny * nz)), 1.0)
    if last:
        for k in range(5):
            value = state[k] + jnp.broadcast_to(offset, (nx, ny * nz)) if k == 0 else state[k]
            for y in range(ny):
                fields[pl.ds(k * nx * ny + y, nx, stride=ny), :] = value[:, y * nz : (y + 1) * nz]
    along_x, along_y = coef[1:2, :], coef[2:3, :]
    upward = coef[4:5, :] > 0.0
    first_y = jnp.where(upward, along_y, 0.0)
    final_y = jnp.where(upward, 0.0, along_y)
    for x in range(nx):
        columns = (mix[x * KROWS : (x + 1) * KROWS, :] * scale).T
        high, low = split(columns)
        lhs = jnp.concatenate([high, low, high], axis=1)
        add = dot(lhs, wmat[...], ((1,), (0,)))
        pieces = []
        for y in range(ny):
            piece = g[x, y] + add[y * nz : (y + 1) * nz]
            outer = None
            if y == 0:
                outer = first_y * yhalo[x]
            if y == ny - 1:
                outer = final_y * yhalo[x]
            if x == 0:
                edge = jnp.concatenate([along_x[:, :half] * xbefore[y], jnp.zeros((nz, half), f32)], axis=1)
                outer = edge if outer is None else outer + edge
            if x == nx - 1:
                edge = jnp.concatenate([jnp.zeros((nz, half), f32), along_x[:, half:] * xafter[y]], axis=1)
                outer = edge if outer is None else outer + edge
            if outer is not None:
                piece = piece + outer * jnp.concatenate([fluid[x, y]] * (nv // LANES), axis=1)
            pieces.append(piece)
        plane = jnp.concatenate(pieces, axis=0)
        h[x] = plane.reshape(ny, nz, nv)
        if last:
            if x:
                copies[x - 1].start()
        else:
            out = local_moments(proj[...], plane)
            mom[pl.ds(x, MOMENTS, stride=nx), :] = out[:MOMENTS]
            ysend[x] = jnp.where(upward, plane[(ny - 1) * nz :], plane[:nz])
            if x == nx - 1:
                xup[...] = h[x, :, :, :half]
            if x == 0:
                xdown[...] = h[x, :, :, half:]
    if last:
        copies[nx - 1].start()
        for copy in copies:
            copy.wait()


def update(target, g, mix, wmat, proj, coef, fluid, halos, mass, far, state, cells):
    nx, ny, nz, nv = g.shape
    last = state is not None
    shapes = [jax.ShapeDtypeStruct(g.shape, f32)]
    if last:
        shapes.append(jax.ShapeDtypeStruct((5 * nx * ny, nz), f32))
    else:
        shapes += [
            jax.ShapeDtypeStruct((MOMENTS * nx, ny * nz), f32),
            jax.ShapeDtypeStruct((nx, nz, nv), f32),
            jax.ShapeDtypeStruct((ny, nz, nv // 2), f32),
            jax.ShapeDtypeStruct((ny, nz, nv // 2), f32),
        ]
    operands = [target, g, mix, wmat, proj, coef, fluid, *halos, mass, far]
    if last:
        operands.append(state)
    vmem = pl.BlockSpec(memory_space=pltpu.VMEM)
    return pl.pallas_call(
        functools.partial(update_kernel, last=last, cells=cells),
        in_specs=[vmem] * len(operands),
        out_shape=shapes,
        out_specs=[pl.BlockSpec(memory_space=pltpu.HBM), vmem] if last else [vmem] * len(shapes),
        scratch_shapes=[pltpu.VMEM(g.shape, f32), pltpu.SemaphoreType.DMA((nx,))] if last else [],
        name="update",
        compiler_params=pltpu.CompilerParams(vmem_limit_bytes=14 << 20),
    )(*operands)


def ring(value, axis, step):
    count = lax.axis_size(axis)
    return lax.ppermute(value, axis, [(i, (i + step) % count) for i in range(count)])


def on_device(initial, velocity, weights, wall, wall_temp, mass_target):
    nx, ny, nz, nv = initial.shape
    width = ny * nz
    n_tx, n_ty, n_vel = (lax.axis_size(a) for a in ("tx", "ty", "vel"))
    if n_ty != 2 or n_tx < 3 or nx <= MACRO_STEPS or width != LANES or n_vel & (n_vel - 1):
        raise ValueError("unsupported sizes")
    cells = float(nx * width * n_tx * n_ty)
    top = n_vel // 2

    def plane_pair(value, flip_y, flip_v):
        pairs = []
        for y in range(n_ty):
            for v in range(n_vel):
                pairs.append((y * n_vel + v, (y ^ flip_y) * n_vel + (v ^ flip_v)))
        return lax.ppermute(value, ("ty", "vel"), pairs)

    h, mom, proj, wmat, coef, ysend, xup, xdown, target = prepare(
        initial, velocity, weights, mass_target[None], float(nv * n_vel)
    )
    for iteration in range(ITERS):
        last = iteration == ITERS - 1
        bit = 1
        while bit < top:
            mom = mom + plane_pair(mom, 0, bit)
            bit *= 2
        across = plane_pair(mom, 0, top)
        beside = plane_pair(mom, 1, 0)
        corner = plane_pair(mom, 1, top)
        yhalo = ring(ysend, "ty", 1)
        xbefore = ring(xup, "tx", 1)
        xafter = ring(xdown, "tx", -1)
        both, sums = join(mom, across, beside, corner, nx)
        left = ring(both, "tx", 1)
        right = ring(both, "tx", -1)
        far = None
        for d in range(2, n_tx - 1):
            part = ring(sums, "tx", d)
            far = part if far is None else far + part
        if far is None:
            far = jnp.zeros_like(sums)
        if iteration == 0:
            fluid_rows, heat, fluid_cells = walls(wall, wall_temp)
        g = stream(h, coef, fluid_cells)
        mix, state, mass = macro(both, left, right, fluid_rows, heat, nz)
        halos = (yhalo, xbefore, xafter)
        outs = update(target, g, mix, wmat, proj, coef, fluid_cells, halos, mass, far, state if last else None, cells)
        h = outs[0]
        if not last:
            mom, ysend, xup, xdown = outs[1:]
    return h, outs[1].reshape(5, nx, ny, nz)


def solution(mesh):
    placed = (
        P("tx", "ty", None, "vel"),
        P(None, "vel"),
        P("vel"),
        P("tx", "ty", None),
        P("tx", "ty", None),
        P(),
    )
    return jax.shard_map(
        on_device,
        mesh=mesh,
        in_specs=placed,
        out_specs=(P("tx", "ty", None, "vel"), P(None, "tx", "ty", None)),
        check_vma=False,
    )
```

```python
import functools

import jax
import jax.numpy as jnp
from jax import lax
from jax.experimental import pallas as pl
from jax.experimental.pallas import tpu as pltpu
from jax.sharding import PartitionSpec as P


ITERS = 3
MACRO_STEPS = 4
REACH = MACRO_STEPS + 1

STEP_TIME = 0.1
COLLISION = 1.0
MACRO_TIME = 0.1
VISCOSITY = 1.0
CONDUCTION = 1.0

LANES = 128
MOMENTS = 14
PROWS = 16
KROWS = 48
f32 = jnp.float32
bf16 = jnp.bfloat16


def split(value):
    high = value.astype(bf16)
    return high, (value - high.astype(f32)).astype(bf16)


def dot(a, b, contract):
    return lax.dot_general(a, b, (contract, ((), ())), preferred_element_type=f32)


def local_moments(proj, plane):
    high, low = split(plane)
    both = dot(proj, high, ((1,), (1,)))
    return both[:PROWS] + both[PROWS:] + dot(proj[:PROWS], low, ((1,), (1,)))


def prepare_kernel(
    vel_far, wgt_far, target_far, source, h, mom, proj, wmat, coef, ysend, xup, xdown, goal, rows, vel, wgt, target, arrived, *, total
):
    planes, ny, nz, nv = source.shape
    order = [planes - 1, *range(planes - 1)]
    copies = [pltpu.make_async_copy(source.at[x], h.at[x], arrived.at[x]) for x in range(planes)]
    small = [
        pltpu.make_async_copy(far, near, arrived.at[planes + i])
        for i, (far, near) in enumerate([(vel_far, vel), (wgt_far, wgt), (target_far, target)])
    ]
    for copy in small:
        copy.start()
    for x in order:
        copies[x].start()
    for copy in small:
        copy.wait()
    goal[...] = jnp.full(goal.shape, target[0], f32)
    vx, vy, vz = vel[0:1, :], vel[1:2, :], vel[2:3, :]

    speed = vx * vx + vy * vy + vz * vz
    scale = wgt[...].reshape(1, nv) / total
    one = jnp.ones_like(speed)
    zero = jnp.zeros_like(speed)
    table = [
        one,
        vx,
        vy,
        vz,
        2.0 / 3.0 * speed - 1.0,
        2.0 * (vx * vx - speed / 3.0),
        2.0 * (vy * vy - speed / 3.0),
        2.0 * (vz * vz - speed / 3.0),
        2.0 * vx * vy,
        2.0 * vx * vz,
        2.0 * vy * vz,
        vx * (speed - 2.5),
        vy * (speed - 2.5),
        vz * (speed - 2.5),
    ]
    for k, row in enumerate(table):
        rows[k : k + 1, :] = row * scale
    for k in range(MOMENTS, PROWS):
        rows[k : k + 1, :] = zero
    high, low = split(rows[0:PROWS, :])
    proj[0:PROWS, :] = high
    proj[PROWS : 2 * PROWS, :] = low
    along_x, along_y, along_z = (STEP_TIME * jnp.abs(v) for v in (vx, vy, vz))
    centre = (1.0 - STEP_TIME * COLLISION) - (along_x + along_y + along_z)
    for k, row in enumerate([centre, along_x, along_y, along_z, vy, vz, zero, zero]):
        coef[k : k + 1, :] = row
    basis = [one, 2.0 * vx, 2.0 * vy, 2.0 * vz, speed - 1.5]
    parts = [
        centre,
        jnp.where(vx > 0.0, along_x, 0.0),
        jnp.where(vx > 0.0, 0.0, along_x),
        jnp.where(vy > 0.0, along_y, 0.0),
        jnp.where(vy > 0.0, 0.0, along_y),
        jnp.where(vz > 0.0, along_z, 0.0),
        jnp.where(vz > 0.0, 0.0, along_z),
        STEP_TIME * COLLISION * one,
    ]
    for i, part in enumerate(parts):
        for k, row in enumerate(basis):
            rows[5 * i + k : 5 * i + k + 1, :] = part * row
    rows[40:41, :] = one
    rows[41:42, :] = basis[4]
    for k in range(42, KROWS):
        rows[k : k + 1, :] = zero
    high, low = split(rows[...])
    wmat[0:KROWS, :] = high
    wmat[KROWS : 2 * KROWS, :] = high
    wmat[2 * KROWS : 3 * KROWS, :] = low

    for x in order:
        copies[x].wait()
        plane = h[x].reshape(ny * nz, nv)
        out = local_moments(proj[...], plane)
        mom[pl.ds(x, MOMENTS, stride=planes), :] = out[:MOMENTS]
        ysend[x] = jnp.where(vy > 0.0, plane[(ny - 1) * nz :], plane[:nz])
        if x == planes - 1:
            xup[...] = h[x, :, :, : nv // 2]
        if x == 0:
            xdown[...] = h[x, :, :, nv // 2 :]


def prepare(initial, velocity, weights, target, total):
    nx, ny, nz, nv = initial.shape
    return pl.pallas_call(
        functools.partial(prepare_kernel, total=total),
        in_specs=[pl.BlockSpec(memory_space=pltpu.HBM)] * 4,
        out_shape=[
            jax.ShapeDtypeStruct(initial.shape, f32),
            jax.ShapeDtypeStruct((MOMENTS * nx, ny * nz), f32),
            jax.ShapeDtypeStruct((2 * PROWS, nv), bf16),
            jax.ShapeDtypeStruct((3 * KROWS, nv), bf16),
            jax.ShapeDtypeStruct((8, nv), f32),
            jax.ShapeDtypeStruct((nx, nz, nv), f32),
            jax.ShapeDtypeStruct((ny, nz, nv // 2), f32),
            jax.ShapeDtypeStruct((ny, nz, nv // 2), f32),
            jax.ShapeDtypeStruct((8, LANES), f32),
        ],
        scratch_shapes=[
            pltpu.VMEM((KROWS, nv), f32),
            pltpu.VMEM(velocity.shape, f32),
            pltpu.VMEM(weights.shape, f32),
            pltpu.SMEM((1,), f32),
            pltpu.SemaphoreType.DMA((nx + 3,)),
        ],
        name="prepare",
        compiler_params=pltpu.CompilerParams(vmem_limit_bytes=12 << 20),
    )(*(pltpu.with_memory_space_constraint(v, pltpu.HBM) for v in (velocity, weights)), target, pltpu.with_memory_space_constraint(initial, pltpu.HBM))


def walls_kernel(wall, wall_temp, rows, heat, cells):
    nx, ny, nz = wall.shape
    square = (nz, nz)
    same = lax.broadcasted_iota(jnp.int32, square, 0) == lax.broadcasted_iota(jnp.int32, square, 1)
    for x in range(nx):
        open_cells = jnp.where(wall[x] == 1, 0.0, 1.0)
        temps = wall_temp[x]
        for y in range(ny):
            part = slice(y * nz, (y + 1) * nz)
            rows[x : x + 1, part] = open_cells[y : y + 1]
            heat[x : x + 1, part] = temps[y : y + 1]
            spread = jnp.where(same, jnp.broadcast_to(open_cells[y : y + 1], square), 0.0)
            cells[x, y] = jnp.broadcast_to(jnp.sum(spread, axis=1, keepdims=True), (nz, LANES))


def walls(wall, wall_temp):
    nx, ny, nz = wall.shape
    return pl.pallas_call(
        walls_kernel,
        out_shape=[
            jax.ShapeDtypeStruct((nx, ny * nz), f32),
            jax.ShapeDtypeStruct((nx, ny * nz), f32),
            jax.ShapeDtypeStruct((nx, ny, nz, LANES), f32),
        ],
        name="walls",
        compiler_params=pltpu.CompilerParams(vmem_limit_bytes=6 << 20),
    )(wall, wall_temp)


def y_direction(lanes, nv):
    quarters = {(lanes.start * 4) // nv, ((lanes.stop - 1) * 4) // nv}
    return {q % 2 == 0 for q in quarters}


def stream_kernel(h, coef, fluid, g):
    nx, ny, nz, nv = h.shape
    tiles = nv // LANES
    for j in range(tiles):
        lanes = slice(j * LANES, (j + 1) * LANES)
        forward_x = j < tiles // 2
        row = lambda k: jnp.broadcast_to(coef[k : k + 1, lanes], (nz, LANES))
        centre, along_x, along_y, along_z = (row(k) for k in range(4))
        up_z = row(5) > 0.0
        up_y = row(4) > 0.0
        signs = y_direction(lanes, nv)
        zero = jnp.zeros((nz, LANES), f32)
        for x in range(nx):
            for y in range(ny):
                c = h[x, y, :, lanes]
                beside = x - 1 if forward_x else x + 1
                ux = h[beside, y, :, lanes] if 0 <= beside < nx else None
                before = h[x, y - 1, :, lanes] if y > 0 else None
                after = h[x, y + 1, :, lanes] if y < ny - 1 else None
                if signs == {True}:
                    uy = before
                elif signs == {False}:
                    uy = after
                else:
                    uy = jnp.where(up_y, zero if before is None else before, zero if after is None else after)
                uz = jnp.where(up_z, pltpu.roll(c, 1, 0), pltpu.roll(c, nz - 1, 0))
                out = centre * c + along_z * uz
                if ux is not None:
                    out = out + along_x * ux
                if uy is not None:
                    out = out + along_y * uy
                g[x, y, :, lanes] = out * fluid[x, y]


def stream(h, coef, fluid):
    return pl.pallas_call(
        stream_kernel,
        out_shape=jax.ShapeDtypeStruct(h.shape, f32),
        name="stream",
        compiler_params=pltpu.CompilerParams(vmem_limit_bytes=12 << 20),
    )(h, coef, fluid)


def join_kernel(mom, across, beside, corner, both, mass, ahead, behind):
    rows = mom.shape[0]
    nx = mass.shape[0]
    own = mom[...] + across[...]
    side = beside[...] + corner[...]
    both[0:rows, :] = own
    both[rows:, :] = side
    sums = own[0:nx] + side[0:nx]
    mass[...] = sums
    comps = 2 * MOMENTS
    for r in range(REACH):
        ahead[r * comps : (r + 1) * comps, :] = both[pl.ds(nx - REACH + r, comps, stride=nx), :]
        behind[r * comps : (r + 1) * comps, :] = both[pl.ds(r, comps, stride=nx), :]
    ahead[REACH * comps :, :] = sums
    behind[REACH * comps :, :] = sums


def join(mom, across, beside, corner, nx):
    rows, width = mom.shape
    return pl.pallas_call(
        join_kernel,
        out_shape=[
            jax.ShapeDtypeStruct((2 * rows, width), f32),
            jax.ShapeDtypeStruct((nx, width), f32),
            jax.ShapeDtypeStruct((2 * MOMENTS * REACH + nx, width), f32),
            jax.ShapeDtypeStruct((2 * MOMENTS * REACH + nx, width), f32),
        ],
        name="join",
        compiler_params=pltpu.CompilerParams(vmem_limit_bytes=4 << 20),
    )(mom, across, beside, corner)


def macro_kernel(mid, left, right, fluid, heat, mix, state_out, mass_out, *, nz):
    nx, width = fluid.shape
    blank = jnp.zeros((nx - REACH, width), f32)

    def field(k):
        halves = []
        for c in (k, MOMENTS + k):
            near = pl.ds(c, REACH, stride=2 * MOMENTS)
            halves.append(jnp.concatenate([blank, left[near, :], mid[c * nx : (c + 1) * nx], right[near, :], blank], axis=0))
        return jnp.concatenate(halves, axis=1)

    rows, lanes = 3 * nx, 2 * width
    depth = lax.broadcasted_iota(jnp.int32, (rows, lanes), 1) % nz
    first, final = depth == 0, depth == nz - 1

    def shift(v, direction, offset):
        if direction == 0:
            return pltpu.roll(v, 1 if offset < 0 else rows - 1, 0)
        if direction == 1:
            return pltpu.roll(v, nz if offset < 0 else lanes - nz, 1)
        if offset < 0:
            return jnp.where(first, pltpu.roll(v, lanes - nz + 1, 1), pltpu.roll(v, 1, 1))
        return jnp.where(final, pltpu.roll(v, nz - 1, 1), pltpu.roll(v, lanes - 1, 1))

    def around(v, directions=(0, 1, 2)):
        return {d: (shift(v, d, 1), shift(v, d, -1)) for d in directions}

    def grad(pair):
        return (pair[0] - pair[1]) * 0.5

    def laplace(v, near):
        total = (near[0][0] + near[0][1]) + (near[1][0] + near[1][1]) + (near[2][0] + near[2][1])
        return total - 6.0 * v

    def slope(v, d):
        return grad(around(v, (d,))[d])

    state = [field(k) for k in range(5)]
    kinetic = state
    near = [None] + [around(state[k]) for k in range(1, 5)]
    stress = [field(5 + k) for k in range(9)]
    sums = [
        slope(stress[0], 0) + slope(stress[3], 1) + slope(stress[4], 2),
        slope(stress[3], 0) + slope(stress[1], 1) + slope(stress[5], 2),
        slope(stress[4], 0) + slope(stress[5], 1) + slope(stress[2], 2),
    ]
    flow = slope(stress[6], 0) + slope(stress[7], 1) + slope(stress[8], 2)
    sources = [-0.5 * (sums[i] + VISCOSITY * laplace(state[1 + i], near[1 + i])) for i in range(3)]
    sources.append(-(2.0 / 3.0) * (flow + CONDUCTION * laplace(state[4], near[4])))
    for step in range(MACRO_STEPS):
        if step:
            near = [None] + [around(state[k]) for k in range(1, 5)]
        near[0] = around(state[0])
        div = grad(near[1][0]) + grad(near[2][1]) + grad(near[3][2])
        rates = [-div]
        for i in range(3):
            rates.append(
                -0.5 * (grad(near[0][i]) + grad(near[4][i]))
                + 0.5 * VISCOSITY * laplace(state[1 + i], near[1 + i])
                + sources[i]
            )
        rates.append(-(2.0 / 3.0) * div + 2.0 / 3.0 * CONDUCTION * laplace(state[4], near[4]) + sources[3])
        state = [s + MACRO_TIME * r for s, r in zip(state, rates)]

    edge = 2 * MOMENTS * REACH
    mass = mid[0:nx] + mid[MOMENTS * nx : (MOMENTS + 1) * nx] + left[edge:] + right[edge:]
    mass_out[...] = mass
    is_fluid = fluid[...]

    def centre(v):
        return v[nx : 2 * nx, :width]

    def emit(k, value):
        mix[pl.ds(k, nx, stride=KROWS), :] = value

    change = [s - k for s, k in zip(state, kinetic)]
    for k in range(5):
        emit(k, centre(change[k]) * is_fluid)
        for d in range(3):
            emit(5 + 10 * d + k, centre(shift(change[k], d, -1)) * is_fluid)
            emit(10 + 10 * d + k, centre(shift(change[k], d, 1)) * is_fluid)
        emit(35 + k, centre(state[k]) * is_fluid)
    emit(40, is_fluid)
    emit(41, heat[...] * (1.0 - is_fluid))
    for k in range(42, KROWS):
        emit(k, jnp.zeros((nx, width), f32))
    for k in range(5):
        state_out[k] = centre(state[k])


def macro(mid, left, right, fluid, heat, nz):
    nx, width = fluid.shape
    return pl.pallas_call(
        functools.partial(macro_kernel, nz=nz),
        out_shape=[
            jax.ShapeDtypeStruct((KROWS * nx, width), f32),
            jax.ShapeDtypeStruct((5, nx, width), f32),
            jax.ShapeDtypeStruct((nx, width), f32),
        ],
        name="macro",
        compiler_params=pltpu.CompilerParams(vmem_limit_bytes=8 << 20),
    )(mid, left, right, fluid, heat)


def update_kernel(target, g, mix, wmat, proj, coef, fluid, yhalo, xbefore, xafter, mass, far, *refs, last, cells):
    nx, ny, nz, nv = g.shape
    half = nv // 2
    if last:
        state, result, fields, h, sent = refs
        copies = [pltpu.make_async_copy(h.at[x], result.at[x], sent.at[x]) for x in range(nx)]
    else:
        h, mom, ysend, xup, xdown = refs
    total = mass[...] + far[...]
    total = jnp.sum(jnp.sum(total, axis=0, keepdims=True), axis=1, keepdims=True)
    offset = target[0:1, 0:1] - total / cells
    is_offset = lax.broadcasted_iota(jnp.int32, (KROWS, ny * nz), 0) == 40
    scale = jnp.where(is_offset, jnp.broadcast_to(offset, (KROWS, ny * nz)), 1.0)
    along_x, along_y = coef[1:2, :], coef[2:3, :]
    upward = coef[4:5, :] > 0.0
    first_y = jnp.where(upward, along_y, 0.0)
    final_y = jnp.where(upward, 0.0, along_y)
    for x in range(nx):
        columns = (mix[x * KROWS : (x + 1) * KROWS, :] * scale).T
        high, low = split(columns)
        lhs = jnp.concatenate([high, low, high], axis=1)
        add = dot(lhs, wmat[...], ((1,), (0,)))
        pieces = []
        for y in range(ny):
            piece = g[x, y] + add[y * nz : (y + 1) * nz]
            outer = None
            if y == 0:
                outer = first_y * yhalo[x]
            if y == ny - 1:
                outer = final_y * yhalo[x]
            if x == 0:
                edge = jnp.concatenate([along_x[:, :half] * xbefore[y], jnp.zeros((nz, half), f32)], axis=1)
                outer = edge if outer is None else outer + edge
            if x == nx - 1:
                edge = jnp.concatenate([jnp.zeros((nz, half), f32), along_x[:, half:] * xafter[y]], axis=1)
                outer = edge if outer is None else outer + edge
            if outer is not None:
                piece = piece + outer * jnp.concatenate([fluid[x, y]] * (nv // LANES), axis=1)
            pieces.append(piece)
        plane = jnp.concatenate(pieces, axis=0)
        h[x] = plane.reshape(ny, nz, nv)
        if last:
            if x:
                copies[x - 1].start()
        else:
            out = local_moments(proj[...], plane)
            mom[pl.ds(x, MOMENTS, stride=nx), :] = out[:MOMENTS]
            ysend[x] = jnp.where(upward, plane[(ny - 1) * nz :], plane[:nz])
            if x == nx - 1:
                xup[...] = h[x, :, :, :half]
            if x == 0:
                xdown[...] = h[x, :, :, half:]
    if last:
        copies[nx - 1].start()
        for k in range(5):
            value = state[k] + jnp.broadcast_to(offset, (nx, ny * nz)) if k == 0 else state[k]
            for y in range(ny):
                fields[pl.ds(k * nx * ny + y, nx, stride=ny), :] = value[:, y * nz : (y + 1) * nz]
        for copy in copies:
            copy.wait()


def update(target, g, mix, wmat, proj, coef, fluid, halos, mass, far, state, cells):
    nx, ny, nz, nv = g.shape
    last = state is not None
    shapes = [jax.ShapeDtypeStruct(g.shape, f32)]
    if last:
        shapes.append(jax.ShapeDtypeStruct((5 * nx * ny, nz), f32))
    else:
        shapes += [
            jax.ShapeDtypeStruct((MOMENTS * nx, ny * nz), f32),
            jax.ShapeDtypeStruct((nx, nz, nv), f32),
            jax.ShapeDtypeStruct((ny, nz, nv // 2), f32),
            jax.ShapeDtypeStruct((ny, nz, nv // 2), f32),
        ]
    operands = [target, g, mix, wmat, proj, coef, fluid, *halos, mass, far]
    if last:
        operands.append(state)
    vmem = pl.BlockSpec(memory_space=pltpu.VMEM)
    return pl.pallas_call(
        functools.partial(update_kernel, last=last, cells=cells),
        in_specs=[vmem] * len(operands),
        out_shape=shapes,
        out_specs=[pl.BlockSpec(memory_space=pltpu.HBM), vmem] if last else [vmem] * len(shapes),
        scratch_shapes=[pltpu.VMEM(g.shape, f32), pltpu.SemaphoreType.DMA((nx,))] if last else [],
        name="update",
        compiler_params=pltpu.CompilerParams(vmem_limit_bytes=14 << 20),
    )(*operands)


def ring(value, axis, step):
    count = lax.axis_size(axis)
    return lax.ppermute(value, axis, [(i, (i + step) % count) for i in range(count)])


def on_device(initial, velocity, weights, wall, wall_temp, mass_target):
    nx, ny, nz, nv = initial.shape
    width = ny * nz
    n_tx, n_ty, n_vel = (lax.axis_size(a) for a in ("tx", "ty", "vel"))
    if n_ty != 2 or n_tx < 3 or nx <= MACRO_STEPS or width != LANES or n_vel & (n_vel - 1):
        raise ValueError("unsupported sizes")
    cells = float(nx * width * n_tx * n_ty)
    top = n_vel // 2

    def plane_pair(value, flip_y, flip_v):
        pairs = []
        for y in range(n_ty):
            for v in range(n_vel):
                pairs.append((y * n_vel + v, (y ^ flip_y) * n_vel + (v ^ flip_v)))
        return lax.ppermute(value, ("ty", "vel"), pairs)

    h, mom, proj, wmat, coef, ysend, xup, xdown, target = prepare(
        initial, velocity, weights, mass_target[None], float(nv * n_vel)
    )
    for iteration in range(ITERS):
        last = iteration == ITERS - 1
        bit = 1
        while bit < top:
            mom = mom + plane_pair(mom, 0, bit)
            bit *= 2
        across = plane_pair(mom, 0, top)
        beside = plane_pair(mom, 1, 0)
        corner = plane_pair(mom, 1, top)
        yhalo = ring(ysend, "ty", 1)
        xbefore = ring(xup, "tx", 1)
        xafter = ring(xdown, "tx", -1)
        both, sums, ahead, behind = join(mom, across, beside, corner, nx)
        left = ring(ahead, "tx", 1)
        right = ring(behind, "tx", -1)
        far = None
        for d in range(2, n_tx - 1):
            part = ring(sums, "tx", d)
            far = part if far is None else far + part
        if far is None:
            far = jnp.zeros_like(sums)
        if iteration == 0:
            fluid_rows, heat, fluid_cells = walls(wall, wall_temp)
        g = stream(h, coef, fluid_cells)
        mix, state, mass = macro(both, left, right, fluid_rows, heat, nz)
        halos = (yhalo, xbefore, xafter)
        outs = update(target, g, mix, wmat, proj, coef, fluid_cells, halos, mass, far, state if last else None, cells)
        h = outs[0]
        if not last:
            mom, ysend, xup, xdown = outs[1:]
    return h, outs[1].reshape(5, nx, ny, nz)


def solution(mesh):
    placed = (
        P("tx", "ty", None, "vel"),
        P(None, "vel"),
        P("vel"),
        P("tx", "ty", None),
        P("tx", "ty", None),
        P(),
    )
    return jax.shard_map(
        on_device,
        mesh=mesh,
        in_specs=placed,
        out_specs=(P("tx", "ty", None, "vel"), P(None, "tx", "ty", None)),
        check_vma=False,
    )
```

```python
import functools

import jax
import jax.numpy as jnp
from jax import lax
from jax.experimental import pallas as pl
from jax.experimental.pallas import tpu as pltpu
from jax.sharding import PartitionSpec as P


ITERS = 3
MACRO_STEPS = 4
REACH = MACRO_STEPS + 1

STEP_TIME = 0.1
COLLISION = 1.0
MACRO_TIME = 0.1
VISCOSITY = 1.0
CONDUCTION = 1.0

LANES = 128
MOMENTS = 14
PROWS = 16
KROWS = 48
f32 = jnp.float32
bf16 = jnp.bfloat16


def split(value):
    high = value.astype(bf16)
    return high, (value - high.astype(f32)).astype(bf16)


def dot(a, b, contract):
    return lax.dot_general(a, b, (contract, ((), ())), preferred_element_type=f32)


def local_moments(proj, plane):
    high, low = split(plane)
    both = dot(proj, high, ((1,), (1,)))
    return both[:PROWS] + both[PROWS:] + dot(proj[:PROWS], low, ((1,), (1,)))


def prepare_kernel(
    vel_far, wgt_far, target_far, source, h, mom, proj, wmat, coef, ysend, xup, xdown, goal, rows, vel, wgt, target, arrived, *, total
):
    planes, ny, nz, nv = source.shape
    order = [planes - 1, *range(planes - 1)]
    copies = [pltpu.make_async_copy(source.at[x], h.at[x], arrived.at[x]) for x in range(planes)]
    small = [
        pltpu.make_async_copy(far, near, arrived.at[planes + i])
        for i, (far, near) in enumerate([(vel_far, vel), (wgt_far, wgt), (target_far, target)])
    ]
    for copy in small:
        copy.start()
    for x in order:
        copies[x].start()
    for copy in small:
        copy.wait()
    goal[...] = jnp.full(goal.shape, target[0], f32)
    vx, vy, vz = vel[0:1, :], vel[1:2, :], vel[2:3, :]

    speed = vx * vx + vy * vy + vz * vz
    scale = wgt[...].reshape(1, nv) / total
    one = jnp.ones_like(speed)
    zero = jnp.zeros_like(speed)
    table = [
        one,
        vx,
        vy,
        vz,
        2.0 / 3.0 * speed - 1.0,
        2.0 * (vx * vx - speed / 3.0),
        2.0 * (vy * vy - speed / 3.0),
        2.0 * (vz * vz - speed / 3.0),
        2.0 * vx * vy,
        2.0 * vx * vz,
        2.0 * vy * vz,
        vx * (speed - 2.5),
        vy * (speed - 2.5),
        vz * (speed - 2.5),
    ]
    for k, row in enumerate(table):
        rows[k : k + 1, :] = row * scale
    for k in range(MOMENTS, PROWS):
        rows[k : k + 1, :] = zero
    high, low = split(rows[0:PROWS, :])
    proj[0:PROWS, :] = high
    proj[PROWS : 2 * PROWS, :] = low
    along_x, along_y, along_z = (STEP_TIME * jnp.abs(v) for v in (vx, vy, vz))
    centre = (1.0 - STEP_TIME * COLLISION) - (along_x + along_y + along_z)
    for k, row in enumerate([centre, along_x, along_y, along_z, vy, vz, zero, zero]):
        coef[k : k + 1, :] = row
    basis = [one, 2.0 * vx, 2.0 * vy, 2.0 * vz, speed - 1.5]
    parts = [
        centre,
        jnp.where(vx > 0.0, along_x, 0.0),
        jnp.where(vx > 0.0, 0.0, along_x),
        jnp.where(vy > 0.0, along_y, 0.0),
        jnp.where(vy > 0.0, 0.0, along_y),
        jnp.where(vz > 0.0, along_z, 0.0),
        jnp.where(vz > 0.0, 0.0, along_z),
        STEP_TIME * COLLISION * one,
    ]
    for i, part in enumerate(parts):
        for k, row in enumerate(basis):
            rows[5 * i + k : 5 * i + k + 1, :] = part * row
    rows[40:41, :] = one
    rows[41:42, :] = basis[4]
    for k in range(42, KROWS):
        rows[k : k + 1, :] = zero
    high, low = split(rows[...])
    wmat[0:KROWS, :] = high
    wmat[KROWS : 2 * KROWS, :] = high
    wmat[2 * KROWS : 3 * KROWS, :] = low

    for i, x in enumerate(order):
        if i % 4 == 0:
            for other in order[i : i + 4]:
                copies[other].wait()
        plane = h[x].reshape(ny * nz, nv)
        out = local_moments(proj[...], plane)
        mom[pl.ds(x, MOMENTS, stride=planes), :] = out[:MOMENTS]
        ysend[x] = jnp.where(vy > 0.0, plane[(ny - 1) * nz :], plane[:nz])
        if x == planes - 1:
            xup[...] = h[x, :, :, : nv // 2]
        if x == 0:
            xdown[...] = h[x, :, :, nv // 2 :]


def prepare(initial, velocity, weights, target, total):
    nx, ny, nz, nv = initial.shape
    return pl.pallas_call(
        functools.partial(prepare_kernel, total=total),
        in_specs=[pl.BlockSpec(memory_space=pltpu.HBM)] * 4,
        out_shape=[
            jax.ShapeDtypeStruct(initial.shape, f32),
            jax.ShapeDtypeStruct((MOMENTS * nx, ny * nz), f32),
            jax.ShapeDtypeStruct((2 * PROWS, nv), bf16),
            jax.ShapeDtypeStruct((3 * KROWS, nv), bf16),
            jax.ShapeDtypeStruct((8, nv), f32),
            jax.ShapeDtypeStruct((nx, nz, nv), f32),
            jax.ShapeDtypeStruct((ny, nz, nv // 2), f32),
            jax.ShapeDtypeStruct((ny, nz, nv // 2), f32),
            jax.ShapeDtypeStruct((8, LANES), f32),
        ],
        scratch_shapes=[
            pltpu.VMEM((KROWS, nv), f32),
            pltpu.VMEM(velocity.shape, f32),
            pltpu.VMEM(weights.shape, f32),
            pltpu.SMEM((1,), f32),
            pltpu.SemaphoreType.DMA((nx + 3,)),
        ],
        name="prepare",
        compiler_params=pltpu.CompilerParams(vmem_limit_bytes=12 << 20),
    )(*(pltpu.with_memory_space_constraint(v, pltpu.HBM) for v in (velocity, weights)), target, pltpu.with_memory_space_constraint(initial, pltpu.HBM))


def walls_kernel(wall, wall_temp, rows, heat, cells):
    nx, ny, nz = wall.shape
    square = (nz, nz)
    same = lax.broadcasted_iota(jnp.int32, square, 0) == lax.broadcasted_iota(jnp.int32, square, 1)
    for x in range(nx):
        open_cells = jnp.where(wall[x] == 1, 0.0, 1.0)
        temps = wall_temp[x]
        for y in range(ny):
            part = slice(y * nz, (y + 1) * nz)
            rows[x : x + 1, part] = open_cells[y : y + 1]
            heat[x : x + 1, part] = temps[y : y + 1]
            spread = jnp.where(same, jnp.broadcast_to(open_cells[y : y + 1], square), 0.0)
            cells[x, y] = jnp.broadcast_to(jnp.sum(spread, axis=1, keepdims=True), (nz, LANES))


def walls(wall, wall_temp):
    nx, ny, nz = wall.shape
    return pl.pallas_call(
        walls_kernel,
        out_shape=[
            jax.ShapeDtypeStruct((nx, ny * nz), f32),
            jax.ShapeDtypeStruct((nx, ny * nz), f32),
            jax.ShapeDtypeStruct((nx, ny, nz, LANES), f32),
        ],
        name="walls",
        compiler_params=pltpu.CompilerParams(vmem_limit_bytes=6 << 20),
    )(wall, wall_temp)


def y_direction(lanes, nv):
    quarters = {(lanes.start * 4) // nv, ((lanes.stop - 1) * 4) // nv}
    return {q % 2 == 0 for q in quarters}


def stream_kernel(h, coef, fluid, g):
    nx, ny, nz, nv = h.shape
    tiles = nv // LANES
    for j in range(tiles):
        lanes = slice(j * LANES, (j + 1) * LANES)
        forward_x = j < tiles // 2
        row = lambda k: jnp.broadcast_to(coef[k : k + 1, lanes], (nz, LANES))
        centre, along_x, along_y, along_z = (row(k) for k in range(4))
        up_z = row(5) > 0.0
        up_y = row(4) > 0.0
        signs = y_direction(lanes, nv)
        zero = jnp.zeros((nz, LANES), f32)
        for x in range(nx):
            for y in range(ny):
                c = h[x, y, :, lanes]
                beside = x - 1 if forward_x else x + 1
                ux = h[beside, y, :, lanes] if 0 <= beside < nx else None
                before = h[x, y - 1, :, lanes] if y > 0 else None
                after = h[x, y + 1, :, lanes] if y < ny - 1 else None
                if signs == {True}:
                    uy = before
                elif signs == {False}:
                    uy = after
                else:
                    uy = jnp.where(up_y, zero if before is None else before, zero if after is None else after)
                uz = jnp.where(up_z, pltpu.roll(c, 1, 0), pltpu.roll(c, nz - 1, 0))
                out = centre * c + along_z * uz
                if ux is not None:
                    out = out + along_x * ux
                if uy is not None:
                    out = out + along_y * uy
                g[x, y, :, lanes] = out * fluid[x, y]


def stream(h, coef, fluid):
    return pl.pallas_call(
        stream_kernel,
        out_shape=jax.ShapeDtypeStruct(h.shape, f32),
        name="stream",
        compiler_params=pltpu.CompilerParams(vmem_limit_bytes=12 << 20),
    )(h, coef, fluid)


def join_kernel(mom, across, beside, corner, both, mass, ahead, behind):
    rows = mom.shape[0]
    nx = mass.shape[0]
    own = mom[...] + across[...]
    side = beside[...] + corner[...]
    both[0:rows, :] = own
    both[rows:, :] = side
    sums = own[0:nx] + side[0:nx]
    mass[...] = sums
    comps = 2 * MOMENTS
    for r in range(REACH):
        ahead[r * comps : (r + 1) * comps, :] = both[pl.ds(nx - REACH + r, comps, stride=nx), :]
        behind[r * comps : (r + 1) * comps, :] = both[pl.ds(r, comps, stride=nx), :]
    ahead[REACH * comps :, :] = sums
    behind[REACH * comps :, :] = sums


def join(mom, across, beside, corner, nx):
    rows, width = mom.shape
    return pl.pallas_call(
        join_kernel,
        out_shape=[
            jax.ShapeDtypeStruct((2 * rows, width), f32),
            jax.ShapeDtypeStruct((nx, width), f32),
            jax.ShapeDtypeStruct((2 * MOMENTS * REACH + nx, width), f32),
            jax.ShapeDtypeStruct((2 * MOMENTS * REACH + nx, width), f32),
        ],
        name="join",
        compiler_params=pltpu.CompilerParams(vmem_limit_bytes=4 << 20),
    )(mom, across, beside, corner)


def macro_kernel(mid, left, right, fluid, heat, mix, mass_out, *state_out, nz):
    nx, width = fluid.shape
    blank = jnp.zeros((nx - REACH, width), f32)

    def field(k):
        halves = []
        for c in (k, MOMENTS + k):
            near = pl.ds(c, REACH, stride=2 * MOMENTS)
            halves.append(jnp.concatenate([blank, left[near, :], mid[c * nx : (c + 1) * nx], right[near, :], blank], axis=0))
        return jnp.concatenate(halves, axis=1)

    rows, lanes = 3 * nx, 2 * width
    depth = lax.broadcasted_iota(jnp.int32, (rows, lanes), 1) % nz
    first, final = depth == 0, depth == nz - 1

    def shift(v, direction, offset):
        if direction == 0:
            return pltpu.roll(v, 1 if offset < 0 else rows - 1, 0)
        if direction == 1:
            return pltpu.roll(v, nz if offset < 0 else lanes - nz, 1)
        if offset < 0:
            return jnp.where(first, pltpu.roll(v, lanes - nz + 1, 1), pltpu.roll(v, 1, 1))
        return jnp.where(final, pltpu.roll(v, nz - 1, 1), pltpu.roll(v, lanes - 1, 1))

    def around(v, directions=(0, 1, 2)):
        return {d: (shift(v, d, 1), shift(v, d, -1)) for d in directions}

    def grad(pair):
        return (pair[0] - pair[1]) * 0.5

    def laplace(v, near):
        total = (near[0][0] + near[0][1]) + (near[1][0] + near[1][1]) + (near[2][0] + near[2][1])
        return total - 6.0 * v

    def slope(v, d):
        return grad(around(v, (d,))[d])

    state = [field(k) for k in range(5)]
    kinetic = state
    near = [None] + [around(state[k]) for k in range(1, 5)]
    stress = [field(5 + k) for k in range(9)]
    sums = [
        slope(stress[0], 0) + slope(stress[3], 1) + slope(stress[4], 2),
        slope(stress[3], 0) + slope(stress[1], 1) + slope(stress[5], 2),
        slope(stress[4], 0) + slope(stress[5], 1) + slope(stress[2], 2),
    ]
    flow = slope(stress[6], 0) + slope(stress[7], 1) + slope(stress[8], 2)
    sources = [-0.5 * (sums[i] + VISCOSITY * laplace(state[1 + i], near[1 + i])) for i in range(3)]
    sources.append(-(2.0 / 3.0) * (flow + CONDUCTION * laplace(state[4], near[4])))
    for step in range(MACRO_STEPS):
        if step:
            near = [None] + [around(state[k]) for k in range(1, 5)]
        near[0] = around(state[0])
        div = grad(near[1][0]) + grad(near[2][1]) + grad(near[3][2])
        rates = [-div]
        for i in range(3):
            rates.append(
                -0.5 * (grad(near[0][i]) + grad(near[4][i]))
                + 0.5 * VISCOSITY * laplace(state[1 + i], near[1 + i])
                + sources[i]
            )
        rates.append(-(2.0 / 3.0) * div + 2.0 / 3.0 * CONDUCTION * laplace(state[4], near[4]) + sources[3])
        state = [s + MACRO_TIME * r for s, r in zip(state, rates)]

    edge = 2 * MOMENTS * REACH
    mass = mid[0:nx] + mid[MOMENTS * nx : (MOMENTS + 1) * nx] + left[edge:] + right[edge:]
    mass_out[...] = mass
    is_fluid = fluid[...]

    def centre(v):
        return v[nx : 2 * nx, :width]

    def emit(k, value):
        mix[pl.ds(k, nx, stride=KROWS), :] = value

    change = [s - k for s, k in zip(state, kinetic)]
    for k in range(5):
        emit(k, centre(change[k]) * is_fluid)
        for d in range(3):
            emit(5 + 10 * d + k, centre(shift(change[k], d, -1)) * is_fluid)
            emit(10 + 10 * d + k, centre(shift(change[k], d, 1)) * is_fluid)
        emit(35 + k, centre(state[k]) * is_fluid)
    emit(40, is_fluid)
    emit(41, heat[...] * (1.0 - is_fluid))
    for k in range(42, KROWS):
        emit(k, jnp.zeros((nx, width), f32))
    for out in state_out:
        for k in range(5):
            out[k] = centre(state[k])


def macro(mid, left, right, fluid, heat, nz, last):
    nx, width = fluid.shape
    return pl.pallas_call(
        functools.partial(macro_kernel, nz=nz),
        out_shape=[
            jax.ShapeDtypeStruct((KROWS * nx, width), f32),
            jax.ShapeDtypeStruct((nx, width), f32),
        ]
        + [jax.ShapeDtypeStruct((5, nx, width), f32)] * last,
        name="macro",
        compiler_params=pltpu.CompilerParams(vmem_limit_bytes=8 << 20),
    )(mid, left, right, fluid, heat)


def update_kernel(target, g, mix, wmat, proj, coef, fluid, yhalo, xbefore, xafter, mass, far, *refs, last, cells):
    nx, ny, nz, nv = g.shape
    half = nv // 2
    if last:
        state, result, fields_far, h, fields, sent = refs
        copies = [pltpu.make_async_copy(h.at[x], result.at[x], sent.at[x]) for x in range(nx)]
    else:
        h, mom, ysend, xup, xdown = refs
    total = mass[...] + far[...]
    total = jnp.sum(jnp.sum(total, axis=0, keepdims=True), axis=1, keepdims=True)
    offset = target[0:1, 0:1] - total / cells
    is_offset = lax.broadcasted_iota(jnp.int32, (KROWS, ny * nz), 0) == 40
    scale = jnp.where(is_offset, jnp.broadcast_to(offset, (KROWS, ny * nz)), 1.0)
    if last:
        fields_copy = pltpu.make_async_copy(fields, fields_far, sent.at[nx])
        for k in range(5):
            value = state[k] + jnp.broadcast_to(offset, (nx, ny * nz)) if k == 0 else state[k]
            for y in range(ny):
                fields[pl.ds(k * nx * ny + y, nx, stride=ny), :] = value[:, y * nz : (y + 1) * nz]
    along_x, along_y = coef[1:2, :], coef[2:3, :]
    upward = coef[4:5, :] > 0.0
    first_y = jnp.where(upward, along_y, 0.0)
    final_y = jnp.where(upward, 0.0, along_y)
    for x in range(nx):
        columns = (mix[x * KROWS : (x + 1) * KROWS, :] * scale).T
        high, low = split(columns)
        lhs = jnp.concatenate([high, low, high], axis=1)
        add = dot(lhs, wmat[...], ((1,), (0,)))
        pieces = []
        for y in range(ny):
            piece = g[x, y] + add[y * nz : (y + 1) * nz]
            outer = None
            if y == 0:
                outer = first_y * yhalo[x]
            if y == ny - 1:
                outer = final_y * yhalo[x]
            if x == 0:
                edge = jnp.concatenate([along_x[:, :half] * xbefore[y], jnp.zeros((nz, half), f32)], axis=1)
                outer = edge if outer is None else outer + edge
            if x == nx - 1:
                edge = jnp.concatenate([jnp.zeros((nz, half), f32), along_x[:, half:] * xafter[y]], axis=1)
                outer = edge if outer is None else outer + edge
            if outer is not None:
                piece = piece + outer * jnp.concatenate([fluid[x, y]] * (nv // LANES), axis=1)
            pieces.append(piece)
        plane = jnp.concatenate(pieces, axis=0)
        h[x] = plane.reshape(ny, nz, nv)
        if last:
            if x % 2 == 1:
                if x < 2:
                    fields_copy.start()
                for other in range(x + 1 - 2, x + 1):
                    copies[other].start()
        else:
            out = local_moments(proj[...], plane)
            mom[pl.ds(x, MOMENTS, stride=nx), :] = out[:MOMENTS]
            ysend[x] = jnp.where(upward, plane[(ny - 1) * nz :], plane[:nz])
            if x == nx - 1:
                xup[...] = h[x, :, :, :half]
            if x == 0:
                xdown[...] = h[x, :, :, half:]
    if last:
        for other in range(nx - nx % 2, nx):
            copies[other].start()
        for copy in [fields_copy, *copies]:
            copy.wait()


def update(target, g, mix, wmat, proj, coef, fluid, halos, mass, far, state, cells):
    nx, ny, nz, nv = g.shape
    last = bool(state)
    shapes = [jax.ShapeDtypeStruct(g.shape, f32)]
    if last:
        shapes.append(jax.ShapeDtypeStruct((5 * nx * ny, nz), f32))
    else:
        shapes += [
            jax.ShapeDtypeStruct((MOMENTS * nx, ny * nz), f32),
            jax.ShapeDtypeStruct((nx, nz, nv), f32),
            jax.ShapeDtypeStruct((ny, nz, nv // 2), f32),
            jax.ShapeDtypeStruct((ny, nz, nv // 2), f32),
        ]
    operands = [target, g, mix, wmat, proj, coef, fluid, *halos, mass, far]
    if last:
        operands += state
    vmem = pl.BlockSpec(memory_space=pltpu.VMEM)
    return pl.pallas_call(
        functools.partial(update_kernel, last=last, cells=cells),
        in_specs=[vmem] * len(operands),
        out_shape=shapes,
        out_specs=[pl.BlockSpec(memory_space=pltpu.HBM)] * 2 if last else [vmem] * len(shapes),
        scratch_shapes=[
            pltpu.VMEM(g.shape, f32),
            pltpu.VMEM((5 * nx * ny, nz), f32),
            pltpu.SemaphoreType.DMA((nx + 1,)),
        ]
        if last
        else [],
        name="update",
        compiler_params=pltpu.CompilerParams(vmem_limit_bytes=14 << 20),
    )(*operands)


def ring(value, axis, step):
    count = lax.axis_size(axis)
    return lax.ppermute(value, axis, [(i, (i + step) % count) for i in range(count)])


def on_device(initial, velocity, weights, wall, wall_temp, mass_target):
    nx, ny, nz, nv = initial.shape
    width = ny * nz
    n_tx, n_ty, n_vel = (lax.axis_size(a) for a in ("tx", "ty", "vel"))
    if n_ty != 2 or n_tx < 3 or nx <= MACRO_STEPS or width != LANES or n_vel & (n_vel - 1):
        raise ValueError("unsupported sizes")
    cells = float(nx * width * n_tx * n_ty)
    top = n_vel // 2

    def plane_pair(value, flip_y, flip_v):
        pairs = []
        for y in range(n_ty):
            for v in range(n_vel):
                pairs.append((y * n_vel + v, (y ^ flip_y) * n_vel + (v ^ flip_v)))
        return lax.ppermute(value, ("ty", "vel"), pairs)

    h, mom, proj, wmat, coef, ysend, xup, xdown, target = prepare(
        initial, velocity, weights, mass_target[None], float(nv * n_vel)
    )
    for iteration in range(ITERS):
        last = iteration == ITERS - 1
        bit = 1
        while bit < top:
            mom = mom + plane_pair(mom, 0, bit)
            bit *= 2
        across = plane_pair(mom, 0, top)
        beside = plane_pair(mom, 1, 0)
        corner = plane_pair(mom, 1, top)
        yhalo = ring(ysend, "ty", 1)
        xbefore = ring(xup, "tx", 1)
        xafter = ring(xdown, "tx", -1)
        both, sums, ahead, behind = join(mom, across, beside, corner, nx)
        left = ring(ahead, "tx", 1)
        right = ring(behind, "tx", -1)
        far = None
        for d in range(2, n_tx - 1):
            part = ring(sums, "tx", d)
            far = part if far is None else far + part
        if far is None:
            far = jnp.zeros_like(sums)
        if iteration == 0:
            fluid_rows, heat, fluid_cells = walls(wall, wall_temp)
        g = stream(h, coef, fluid_cells)
        mix, mass, *state = macro(both, left, right, fluid_rows, heat, nz, last)
        halos = (yhalo, xbefore, xafter)
        outs = update(target, g, mix, wmat, proj, coef, fluid_cells, halos, mass, far, state, cells)
        h = outs[0]
        if not last:
            mom, ysend, xup, xdown = outs[1:]
    return h, outs[1].reshape(5, nx, ny, nz)


def solution(mesh):
    placed = (
        P("tx", "ty", None, "vel"),
        P(None, "vel"),
        P("vel"),
        P("tx", "ty", None),
        P("tx", "ty", None),
        P(),
    )
    return jax.shard_map(
        on_device,
        mesh=mesh,
        in_specs=placed,
        out_specs=(P("tx", "ty", None, "vel"), P(None, "tx", "ty", None)),
        check_vma=False,
    )
```
